512 devices in a mesh: row: 16 (over y, core), col: 32 (over z, x).
Axes of the slice: x: 4, y: 8, z: 8, core: 2. Of those that a mesh axis runs over, the one named last changes fastest.
Arguments:
- couplings: float32 [24576, 24576], P('row', 'col'), may hold values from -0.0390625 to 0.0390625
- diag_terms: float32 [24576], P('col'), may hold values from 1 to 4
- start_block: float32 [3, 24576], P(None, 'col'), may hold values from -6 to 6
Outputs:
- basis_scaled: float32 [2, 3, 24576], P(None, None, 'col')
- coeffs: float32 [2, 2, 3, 3], replicated
The draws below stay inside these ranges and needn't reach their ends.
All inputs are finite; a program needn't handle non-finite values.
Results may differ from the reference program's by a relative error of at most 0.0003.
Values sent between devices are 32-bit elements; how exact they have to be, the bound alone decides.
No kernel may reach another device: no remote copies, remote signals or barrier semaphores. Data moves between devices by JAX's collectives and lax.ppermute only.
A program may use at most 64 MiB of HBM per device.

```python
import math
import jax
import jax.numpy as jnp
from jax import lax

RHS = 3
ITERS = 2
M = 24576


def steps_of(stream_key, extent, pieces, low, high):
    def one(position, blocks):
        heights = jax.random.uniform(jax.random.fold_in(jax.random.fold_in(stream_key, 6), position), (blocks,), jnp.float32, low / len(pieces), high / len(pieces))
        return jnp.repeat(jnp.exp(heights), extent[position] // blocks).reshape((-1,) + (1,) * (len(extent) - position - 1))

    factor_of = one(*pieces[0])
    for cut in pieces[1:]:
        factor_of = factor_of * one(*cut)
    return factor_of


def scatter_about(rng, dims, width, reach, pieces=(), kind=jnp.bfloat16):
    drawn = width * jax.random.normal(rng, dims, jnp.float32)
    if pieces:
        drawn = drawn * steps_of(rng, dims, pieces, -0.22, 0.18)
    return jnp.clip(drawn, -reach, reach).astype(kind)


def setup_inputs(seed: int = 0) -> dict:
    key_list = jax.random.split(jax.random.key(seed), 4)
    return {
        "couplings": scatter_about(key_list[0], (M, M), M ** -0.5, 0.0390625, ((0, 16), (1, 32)), jnp.float32),
        "diag_terms": jnp.clip(jnp.exp(math.log(4.0) - 1.3862944 * jax.random.uniform(key_list[1], (M,), jnp.float32) ** steps_of(key_list[1], (M,), ((0, 32),), -0.2, 0.2)), 1.0, 4.0),
        "start_block": scatter_about(key_list[2], (RHS, M), 1.0, 6.0, ((1, 32),), jnp.float32),
    }


def product(a, b):
    return jnp.dot(a.astype(jnp.float32), b.astype(jnp.float32), precision=lax.Precision.HIGHEST, preferred_element_type=jnp.float32)

def orthonormal(block):
    gram_matrix = product(block, block.T)
    factor = jnp.linalg.cholesky(gram_matrix)
    return (jax.scipy.linalg.solve_triangular(factor, block, lower=True), factor)

def reference(couplings, diag_terms, start_block):
    current, first_factor = orthonormal(start_block)
    basis = [current]
    scaled = []
    blocks = []
    root = jnp.sqrt(jnp.float32(M))
    for step in range(ITERS):
        forward = product(couplings, current.T).T
        backward = product(current, couplings)
        image = diag_terms[None, :] * current + 0.5 * (forward + backward)
        prior = jnp.concatenate(basis, 0)
        correlation = product(image, prior.T)
        image = image - product(correlation, prior)
        current, factor = orthonormal(image)
        basis.append(current)
        scaled.append(current * root)
        blocks.append(jnp.stack([correlation[:, 3 * step:3 * step + 3], factor]))
    return (jnp.stack(scaled), jnp.stack(blocks))
```

```python
import jax
import jax.numpy as jnp
from jax import lax
from jax.sharding import PartitionSpec as P

M = 24576
SHIFT = 2.0


def product(a, b):
    return jnp.dot(a, b, precision=lax.Precision.HIGHEST, preferred_element_type=jnp.float32)


def product_rows(a, matrix):
    return lax.dot_general(
        a,
        matrix,
        (((1,), (1,)), ((), ())),
        precision=lax.Precision.HIGHEST,
        preferred_element_type=jnp.float32,
    )


def shards(couplings, diag_terms, start_block):
    row_index = lax.axis_index("row")
    width = couplings.shape[1]
    flat = 3 * width
    cols = lax.axis_size("col")
    rows = lax.axis_size("row")
    shifted = diag_terms - SHIFT

    def exchange(block, extra):
        halves = jnp.moveaxis(product_rows(block, couplings).reshape(3, 2, width), 1, 0).reshape(2, flat)
        slot = lax.broadcasted_iota(jnp.int32, (cols, 1), 0)
        aimed = jnp.where(slot // 2 == row_index, jnp.tile(halves, (cols // 2, 1)), 0.0)
        parts = [jnp.broadcast_to(block.reshape(1, flat), (cols, flat)), aimed]
        if extra is not None:
            padded = jnp.pad(extra, (0, 128 - extra.shape[0]))
            parts.append(jnp.broadcast_to(padded[None], (cols, 128)))
        sent = jnp.concatenate(parts, 1)[:, None, :]
        got = lax.all_to_all(sent, "col", 0, 0, tiled=True)[:, 0, :]
        mine = lax.dynamic_slice(got, (2 * row_index, 0), (2, flat)).reshape(2, 3, width)
        tail = jnp.sum(got[:, flat:], axis=0)
        return jnp.moveaxis(mine, 0, 1).reshape(3, 2 * width), tail

    def collect(block, own_rows, forward):
        part = 0.5 * (product(own_rows, couplings) + forward)
        sent = jnp.broadcast_to(part.reshape(1, 1, flat), (rows, 1, flat))
        got = lax.all_to_all(sent, "row", 0, 0, tiled=True)
        return jnp.sum(got, axis=0).reshape(3, width) + shifted[None] * block

    def inverse(lower):
        return jax.scipy.linalg.solve_triangular(lower, jnp.eye(3, dtype=jnp.float32), lower=True)

    own_rows, tail = exchange(start_block, None)
    z1 = collect(start_block, own_rows, tail.reshape(3, width))
    both = jnp.concatenate([start_block, z1], 0)
    gram = product(both, both.T)
    own_rows, tail = exchange(z1, gram.reshape(-1))
    gram = tail[flat : flat + 36].reshape(6, 6)
    n0 = inverse(jnp.linalg.cholesky(gram[:3, :3]))
    c0 = product(product(n0, gram[:3, 3:]), n0.T)
    c0 = product(n0, product(n0, gram[3:, :3]).T).T
    h1 = product(product(n0, gram[3:, 3:]), n0.T) - product(c0, c0.T)
    l1 = jnp.linalg.cholesky(0.5 * (h1 + h1.T))
    n1 = inverse(l1)
    y2 = collect(z1, own_rows, tail[:flat].reshape(3, width))
    q0 = product(n0, start_block)
    u = product(n0, z1)
    q1 = product(n1, u - product(c0, q0))
    w = product(n1, product(n0, y2) - product(c0, u))
    w = w - product(l1.T, q0) - product(c0, q1)
    three = jnp.concatenate([q0, q1, w], 0)
    last = product(w, three.T)
    sent = jnp.broadcast_to(jnp.pad(last.reshape(-1), (0, 101))[None, None], (cols, 1, 128))
    last = jnp.sum(lax.all_to_all(sent, "col", 0, 0, tiled=True), axis=(0, 1))[:27].reshape(3, 9)
    d0, d1, h2 = last[:, :3], last[:, 3:6], last[:, 6:]
    h2 = h2 - product(d0, d0.T) - product(d1, d1.T)
    l2 = jnp.linalg.cholesky(0.5 * (h2 + h2.T))
    q2 = product(inverse(l2), w - product(d0, q0) - product(d1, q1))
    root = jnp.sqrt(jnp.float32(M))
    shift = SHIFT * jnp.eye(3, dtype=jnp.float32)
    coeffs = jnp.stack([jnp.stack([c0 + shift, l1]), jnp.stack([c0 + d1 + shift, l2])])
    return jnp.stack([q1, q2]) * root, coeffs


def solution(mesh):
    placed = (P("row", "col"), P("col"), P(None, "col"))
    return jax.shard_map(
        shards, mesh=mesh, in_specs=placed, out_specs=(P(None, None, "col"), P()), check_vma=False
    )
```

```python
import jax
import jax.numpy as jnp
from jax import lax
from jax.experimental import pallas as pl
from jax.experimental.pallas import tpu as pltpu
from jax.sharding import PartitionSpec as P

M = 24576
SHIFT = 2.5
W = 768
FLAT = 3 * W
CHUNK = 256
F32 = jnp.float32
BF16 = jnp.bfloat16
VMEM = pl.BlockSpec(memory_space=pltpu.VMEM)


def in_vmem(shape, dtype=F32):
    return pltpu.VMEM(shape, dtype)


def three_parts(x):
    first = x.astype(BF16).astype(F32)
    rest = x - first
    second = rest.astype(BF16).astype(F32)
    return jnp.concatenate([first, second, rest - second], 0).astype(BF16)


def folded(wide):
    return wide[0:8] + wide[8:16] + wide[16:24]


def over_rows(parts, matrix):
    return lax.dot_general(parts, matrix, (((1,), (1,)), ((), ())), preferred_element_type=F32)


def over_cols(parts, matrix):
    return lax.dot_general(parts, matrix, (((1,), (0,)), ((), ())), preferred_element_type=F32)


def rows_of(flat):
    return [flat[:, k * W : (k + 1) * W] for k in range(3)]


def inner(a, b):
    return jnp.sum(a * b, axis=1, keepdims=True)


def packed(values):
    lane = lax.broadcasted_iota(jnp.int32, (1, 128), 1)
    tile = jnp.zeros((1, 128), F32)
    for at, value in enumerate(values):
        tile = jnp.where(lane == at, value, tile)
    return tile


def unpacked(tile, count):
    lane = lax.broadcasted_iota(jnp.int32, (1, 128), 1)
    return [jnp.sum(jnp.where(lane == at, tile, 0.0), axis=1, keepdims=True) for at in range(count)]


def symmetric(six):
    a, b, c, d, e, f = six
    return [[a, b, c], [b, d, e], [c, e, f]]


def times(a, b):
    return [[sum(a[i][k] * b[k][j] for k in range(3)) for j in range(3)] for i in range(3)]


def turned(a):
    return [[a[j][i] for j in range(3)] for i in range(3)]


def minus(a, b):
    return [[a[i][j] - b[i][j] for j in range(3)] for i in range(3)]


def cholesky(h):
    zero = jnp.zeros_like(h[0][0])
    a = jnp.sqrt(h[0][0])
    b = h[1][0] / a
    c = h[2][0] / a
    d = jnp.sqrt(h[1][1] - b * b)
    e = (h[2][1] - c * b) / d
    f = jnp.sqrt(h[2][2] - c * c - e * e)
    return [[a, zero, zero], [b, d, zero], [c, e, f]]


def inverse(low):
    zero = jnp.zeros_like(low[0][0])
    a, d, f = 1.0 / low[0][0], 1.0 / low[1][1], 1.0 / low[2][2]
    b = -low[1][0] * a * d
    e = -low[2][1] * d * f
    c = -(low[2][0] * a + low[2][1] * b) * f
    return [[a, zero, zero], [b, d, zero], [c, e, f]]


def combine(matrix, vectors):
    return [sum(matrix[i][k] * vectors[k] for k in range(3)) for i in range(3)]


def place(row_index, forward_ref, sent_ref):
    for half in range(2):
        for k in range(3):
            sent_ref[2 * row_index + half, :, k * W : (k + 1) * W] = forward_ref[k : k + 1, half * W : (half + 1) * W]


def first_kernel(x_ref, a_ref, sent_ref, high_ref, low_ref, whole, x_rows, forward, sems):
    row_index = lax.axis_index("row")
    pieces = [pl.ds(i * CHUNK, CHUNK) for i in range(2 * W // CHUNK)]
    copies = [pltpu.make_async_copy(a_ref.at[piece], whole.at[piece], sems.at[i]) for i, piece in enumerate(pieces)]
    for copy in copies:
        copy.start()
    x = x_ref[...]
    x_rows[...] = jnp.zeros_like(x_rows)
    for k, row in enumerate(rows_of(x)):
        x_rows[k : k + 1, :] = row
    for p in range(sent_ref.shape[0]):
        sent_ref[p] = x
    parts = three_parts(x_rows[...])
    for copy, piece in zip(copies, pieces):
        copy.wait()
        block = whole[piece, :]
        high = block.astype(BF16)
        low = (block - high.astype(F32)).astype(BF16)
        high_ref[piece, :] = high
        low_ref[piece, :] = low
        forward[:, piece] = 0.5 * folded(over_rows(parts, high) + over_rows(parts, low))
    place(row_index, forward, sent_ref)


def forward_kernel(z_ref, x_ref, high_ref, low_ref, sent_ref, z_rows, forward):
    row_index = lax.axis_index("row")
    z = z_ref[...]
    z_rows[...] = jnp.zeros_like(z_rows)
    for k, row in enumerate(rows_of(z)):
        z_rows[k : k + 1, :] = row
    parts = three_parts(z_rows[...])
    six = rows_of(x_ref[...]) + rows_of(z)
    tile = packed([inner(six[i], six[j]) for i in range(6) for j in range(i, 6)])
    for p in range(sent_ref.shape[0]):
        sent_ref[p, :, 0:FLAT] = z
        sent_ref[p, :, FLAT:] = tile
    forward[...] = 0.5 * folded(over_rows(parts, high_ref[...]) + over_rows(parts, low_ref[...]))
    place(row_index, forward, sent_ref)


def backward_kernel(got_ref, own_ref, cross_ref, high_ref, low_ref, sent_ref, v_rows):
    row_index = lax.axis_index("row")
    col_index = lax.axis_index("col")
    home = col_index // 2 == row_index
    v_rows[...] = jnp.zeros_like(v_rows)
    for half in range(2):
        mine = jnp.where(col_index % 2 == half, own_ref[...], cross_ref[...])
        block = jnp.where(home, mine, got_ref[2 * row_index + half, :, 0:FLAT])
        for k, row in enumerate(rows_of(block)):
            v_rows[k : k + 1, half * W : (half + 1) * W] = row
    parts = three_parts(v_rows[...])
    total = got_ref[0, :, 0:FLAT]
    for p in range(1, got_ref.shape[0]):
        total = total + got_ref[p, :, 0:FLAT]
    total = rows_of(jnp.where(home, total, 0.0))
    back = 0.5 * folded(over_cols(parts, high_ref[...]) + over_cols(parts, low_ref[...]))
    for k in range(3):
        part = back[k : k + 1] + total[k]
        for p in range(sent_ref.shape[0]):
            sent_ref[p, :, k * W : (k + 1) * W] = part


def algebra_kernel(got_ref, coef_ref):
    tile = got_ref[0, :, FLAT:]
    for p in range(1, got_ref.shape[0]):
        tile = tile + got_ref[p, :, FLAT:]
    flat = iter(unpacked(tile, 21))
    gram = {(i, j): next(flat) for i in range(6) for j in range(i, 6)}
    g00 = symmetric([gram[i, j] for i in range(3) for j in range(i, 3)])
    g01 = [[gram[i, j + 3] for j in range(3)] for i in range(3)]
    g11 = symmetric([gram[i + 3, j + 3] for i in range(3) for j in range(i, 3)])
    n0 = inverse(cholesky(g00))
    n0t = turned(n0)
    c0 = times(times(n0, turned(g01)), n0t)
    l1 = cholesky(minus(times(times(n0, g11), n0t), times(c0, turned(c0))))
    n1 = inverse(l1)
    at = 0
    for matrix in (n0, n1, c0, l1):
        for i in range(3):
            for j in range(3):
                coef_ref[at : at + 1, :] = jnp.broadcast_to(matrix[i][j], (1, 128))
                at += 1


def loaded(coef_ref, which, width):
    row = lambda at: coef_ref[at : at + 1, :]
    wide = lambda v: v if width == 128 else jnp.concatenate([v] * (width // 128), 1)
    return [[wide(row(9 * which + 3 * i + j)) for j in range(3)] for i in range(3)]


def residual_kernel(got_ref, z_ref, x_ref, d_ref, coef_ref, sent_ref, basis_ref):
    total = got_ref[0]
    for p in range(1, got_ref.shape[0]):
        total = total + got_ref[p]
    z = z_ref[...]
    y = rows_of(total + d_ref[...] * z)
    n0, n1, c0, l1 = (loaded(coef_ref, i, W) for i in range(4))
    q0 = combine(n0, rows_of(x_ref[...]))
    u = combine(n0, rows_of(z))
    q1 = combine(n1, [a - b for a, b in zip(u, combine(c0, q0))])
    w = combine(n1, [a - b for a, b in zip(combine(n0, y), combine(c0, u))])
    known = [a + b for a, b in zip(combine(turned(l1), q0), combine(c0, q1))]
    w = [a - b for a, b in zip(w, known)]
    values = [inner(a, b) for a in w for b in q0 + q1]
    values += [inner(w[i], w[j]) for i in range(3) for j in range(i, 3)]
    tile = packed(values)
    for p in range(sent_ref.shape[0]):
        sent_ref[p] = tile
    for at, row in enumerate(q0 + q1 + w):
        basis_ref[at : at + 1, :] = row


def last_kernel(got_ref, basis_ref, coef_ref, out_ref, coeffs_ref):
    tile = got_ref[0]
    for p in range(1, got_ref.shape[0]):
        tile = tile + got_ref[p]
    values = unpacked(tile, 24)
    d0 = [values[6 * i : 6 * i + 3] for i in range(3)]
    d1 = [values[6 * i + 3 : 6 * i + 6] for i in range(3)]
    h2 = minus(minus(symmetric(values[18:]), times(d0, turned(d0))), times(d1, turned(d1)))
    l2 = cholesky(h2)
    n2 = inverse(l2)
    rows = [basis_ref[at : at + 1, :] for at in range(9)]
    q0, q1, w = rows[:3], rows[3:6], rows[6:]
    known = [a + b for a, b in zip(combine(d0, q0), combine(d1, q1))]
    q2 = combine(n2, [a - b for a, b in zip(w, known)])
    root = float(M) ** 0.5
    for k in range(3):
        out_ref[0, k : k + 1, :] = q1[k] * root
        out_ref[1, k : k + 1, :] = q2[k] * root
    c0, l1 = ([[v[:, 0:1] for v in line] for line in loaded(coef_ref, i, 128)] for i in (2, 3))
    down = lax.broadcasted_iota(jnp.int32, (3, 3), 0)
    across = lax.broadcasted_iota(jnp.int32, (3, 3), 1)

    def square(matrix, shift):
        tile = jnp.where(down == across, shift, 0.0)
        for i in range(3):
            for j in range(3):
                tile = jnp.where((down == i) & (across == j), tile + matrix[i][j], tile)
        return tile

    second = [[c0[i][j] + d1[i][j] for j in range(3)] for i in range(3)]
    coeffs_ref[0, 0] = square(c0, SHIFT)
    coeffs_ref[0, 1] = square(l1, 0.0)
    coeffs_ref[1, 0] = square(second, SHIFT)
    coeffs_ref[1, 1] = square(l2, 0.0)


def call(kernel, out, inputs, scratch=(), specs=None, flops=2_000_000):
    return pl.pallas_call(
        kernel,
        out_shape=out,
        in_specs=specs or [VMEM] * len(inputs),
        out_specs=jax.tree.map(lambda _: VMEM, out),
        scratch_shapes=list(scratch),
        cost_estimate=pl.CostEstimate(flops=flops, bytes_accessed=100_000, transcendentals=0),
        name=kernel.__name__,
        compiler_params=pltpu.CompilerParams(vmem_limit_bytes=24 << 20),
    )(*inputs)


def shards(couplings, diag_terms, start_block):
    cols = lax.axis_size("col")
    rows = lax.axis_size("row")
    x = start_block.reshape(1, FLAT)
    d = jnp.tile(diag_terms - SHIFT, 3).reshape(1, FLAT)
    swap = [(i, i ^ 1) for i in range(cols)]
    whole = (2 * W, W)
    f32 = lambda *shape: jax.ShapeDtypeStruct(shape, F32)

    def swapped(block):
        return lax.ppermute(block, "col", swap)

    def collect(got, own, cross):
        sent = call(
            backward_kernel,
            f32(rows, 1, FLAT),
            (got, own, cross, high, low),
            [pltpu.VMEM((8, 2 * W), F32)],
        )
        return lax.all_to_all(sent, "row", 0, 0, tiled=True)

    cross = swapped(x)
    sent, high, low = call(
        first_kernel,
        (f32(cols, 1, FLAT), in_vmem(whole, BF16), in_vmem(whole, BF16)),
        (x, couplings),
        [
            pltpu.VMEM(whole, F32),
            pltpu.VMEM((8, W), F32),
            pltpu.VMEM((8, 2 * W), F32),
            pltpu.SemaphoreType.DMA((2 * W // CHUNK,)),
        ],
        [VMEM, pl.BlockSpec(memory_space=pl.ANY)],
    )
    got = lax.all_to_all(sent, "col", 0, 0, tiled=True)
    got = collect(got, x, cross)
    z = jnp.sum(got, axis=0) + d * x
    cross = swapped(z)
    sent = call(
        forward_kernel,
        f32(cols, 1, FLAT + 128),
        (z, x, high, low),
        [pltpu.VMEM((8, W), F32), pltpu.VMEM((8, 2 * W), F32)],
    )
    got = lax.all_to_all(sent, "col", 0, 0, tiled=True)
    coef = call(algebra_kernel, f32(40, 128), (got,))
    got = collect(got, z, cross)
    sent, basis = call(residual_kernel, (f32(cols, 1, 128), f32(16, W)), (got, z, x, d, coef))
    got = lax.all_to_all(sent, "col", 0, 0, tiled=True)
    return call(last_kernel, (f32(2, 3, W), f32(2, 2, 3, 3)), (got, basis, coef))


def solution(mesh):
    placed = (P("row", "col"), P("col"), P(None, "col"))
    return jax.shard_map(
        shards, mesh=mesh, in_specs=placed, out_specs=(P(None, None, "col"), P()), check_vma=False
    )
```

```python
import jax
import jax.numpy as jnp
from jax import lax
from jax.experimental import pallas as pl
from jax.experimental.pallas import tpu as pltpu
from jax.sharding import PartitionSpec as P

M = 24576
SHIFT = 2.5
W = 768
FLAT = 3 * W
CHUNK = 256
F32 = jnp.float32
BF16 = jnp.bfloat16
VMEM = pl.BlockSpec(memory_space=pltpu.VMEM)
HBM = pl.BlockSpec(memory_space=pltpu.HBM)


def in_vmem(shape, dtype=F32):
    return pltpu.VMEM(shape, dtype)


def three_parts(x):
    first = x.astype(BF16).astype(F32)
    rest = x - first
    second = rest.astype(BF16).astype(F32)
    return jnp.concatenate([first, second, rest - second], 0).astype(BF16)


def folded(wide):
    return wide[0:8] + wide[8:16] + wide[16:24]


def over_rows(parts, matrix):
    return lax.dot_general(parts, matrix, (((1,), (1,)), ((), ())), preferred_element_type=F32)


def over_cols(parts, matrix):
    return lax.dot_general(parts, matrix, (((1,), (0,)), ((), ())), preferred_element_type=F32)


def rows_of(flat):
    return [flat[:, k * W : (k + 1) * W] for k in range(3)]


def inner(a, b):
    return jnp.sum(a * b, axis=1, keepdims=True)


def packed(values):
    lane = lax.broadcasted_iota(jnp.int32, (1, 128), 1)
    tile = jnp.zeros((1, 128), F32)
    for at, value in enumerate(values):
        tile = jnp.where(lane == at, value, tile)
    return tile


def unpacked(tile, count):
    lane = lax.broadcasted_iota(jnp.int32, (1, 128), 1)
    return [jnp.sum(jnp.where(lane == at, tile, 0.0), axis=1, keepdims=True) for at in range(count)]


def symmetric(six):
    a, b, c, d, e, f = six
    return [[a, b, c], [b, d, e], [c, e, f]]


def times(a, b):
    return [[sum(a[i][k] * b[k][j] for k in range(3)) for j in range(3)] for i in range(3)]


def turned(a):
    return [[a[j][i] for j in range(3)] for i in range(3)]


def minus(a, b):
    return [[a[i][j] - b[i][j] for j in range(3)] for i in range(3)]


def cholesky(h):
    zero = jnp.zeros_like(h[0][0])
    a = jnp.sqrt(h[0][0])
    b = h[1][0] / a
    c = h[2][0] / a
    d = jnp.sqrt(h[1][1] - b * b)
    e = (h[2][1] - c * b) / d
    f = jnp.sqrt(h[2][2] - c * c - e * e)
    return [[a, zero, zero], [b, d, zero], [c, e, f]]


def inverse(low):
    zero = jnp.zeros_like(low[0][0])
    a, d, f = 1.0 / low[0][0], 1.0 / low[1][1], 1.0 / low[2][2]
    b = -low[1][0] * a * d
    e = -low[2][1] * d * f
    c = -(low[2][0] * a + low[2][1] * b) * f
    return [[a, zero, zero], [b, d, zero], [c, e, f]]


def combine(matrix, vectors):
    return [sum(matrix[i][k] * vectors[k] for k in range(3)) for i in range(3)]


def place(row_index, forward_ref, sent_ref):
    for half in range(2):
        for k in range(3):
            sent_ref[2 * row_index + half, :, k * W : (k + 1) * W] = forward_ref[k : k + 1, half * W : (half + 1) * W]


def first_kernel(x_ref, a_ref, sent_ref, flat_ref, high_ref, low_ref, whole, low, x_rows, forward, sems, out_sems):
    row_index = lax.axis_index("row")
    pieces = [pl.ds(i * CHUNK, CHUNK) for i in range(2 * W // CHUNK)]
    copies = [pltpu.make_async_copy(a_ref.at[piece], whole.at[piece], sems.at[i]) for i, piece in enumerate(pieces)]
    leaving = [pltpu.make_async_copy(low.at[piece], low_ref.at[piece], out_sems.at[i]) for i, piece in enumerate(pieces)]
    for copy in copies:
        copy.start()
    x_rows[...] = jnp.zeros_like(x_rows)
    x_rows[0:3, :] = x_ref[...]
    for k in range(3):
        flat_ref[:, k * W : (k + 1) * W] = x_ref[k : k + 1, :]
    x = flat_ref[...]
    for p in range(sent_ref.shape[0]):
        sent_ref[p] = x
    parts = three_parts(x_rows[...])
    for i, piece in enumerate(pieces):
        copies[i].wait()
        block = whole[piece, :]
        high = block.astype(BF16)
        rest = (block - high.astype(F32)).astype(BF16)
        high_ref[piece, :] = high
        low[piece, :] = rest
        leaving[i].start()
        forward[:, piece] = 0.5 * folded(over_rows(parts, high) + over_rows(parts, rest))
    place(row_index, forward, sent_ref)
    for copy in leaving:
        copy.wait()


def fetch(low_ref, low, sems):
    step = low.shape[0] // sems.shape[0]
    pieces = [pl.ds(i * step, step) for i in range(sems.shape[0])]
    copies = [pltpu.make_async_copy(low_ref.at[piece], low.at[piece], sems.at[i]) for i, piece in enumerate(pieces)]
    for copy in copies:
        copy.start()
    return list(zip(copies, pieces))


def forward_kernel(z_ref, x_ref, high_ref, low_ref, sent_ref, low, z_rows, forward, sems):
    row_index = lax.axis_index("row")
    copies = fetch(low_ref, low, sems)
    z = z_ref[...]
    z_rows[...] = jnp.zeros_like(z_rows)
    for k, row in enumerate(rows_of(z)):
        z_rows[k : k + 1, :] = row
    parts = three_parts(z_rows[...])
    six = rows_of(x_ref[...]) + rows_of(z)
    tile = packed([inner(six[i], six[j]) for i in range(6) for j in range(i, 6)])
    for p in range(sent_ref.shape[0]):
        sent_ref[p, :, 0:FLAT] = z
        sent_ref[p, :, FLAT:] = tile
    forward[...] = folded(over_rows(parts, high_ref[...]))
    for copy, piece in copies:
        copy.wait()
        forward[:, piece] = 0.5 * (forward[:, piece] + folded(over_rows(parts, low[piece, :])))
    place(row_index, forward, sent_ref)


def backward_kernel(got_ref, own_ref, cross_ref, high_ref, low_ref, sent_ref, low, v_rows, sems):
    copies = fetch(low_ref, low, sems)
    row_index = lax.axis_index("row")
    col_index = lax.axis_index("col")
    home = col_index // 2 == row_index
    v_rows[...] = jnp.zeros_like(v_rows)
    for half in range(2):
        mine = jnp.where(col_index % 2 == half, own_ref[...], cross_ref[...])
        block = jnp.where(home, mine, got_ref[2 * row_index + half, :, 0:FLAT])
        for k, row in enumerate(rows_of(block)):
            v_rows[k : k + 1, half * W : (half + 1) * W] = row
    parts = three_parts(v_rows[...])
    total = got_ref[0, :, 0:FLAT]
    for p in range(1, got_ref.shape[0]):
        total = total + got_ref[p, :, 0:FLAT]
    total = rows_of(jnp.where(home, total, 0.0))
    wide = over_cols(parts, high_ref[...])
    for i, (copy, piece) in enumerate(copies):
        copy.wait()
        step = low.shape[0] // len(copies)
        wide = wide + over_cols(parts[:, i * step : (i + 1) * step], low[piece, :])
    back = 0.5 * folded(wide)
    for k in range(3):
        part = back[k : k + 1] + total[k]
        for p in range(sent_ref.shape[0]):
            sent_ref[p, :, k * W : (k + 1) * W] = part


def algebra_kernel(got_ref, coef_ref):
    tile = got_ref[0, :, FLAT:]
    for p in range(1, got_ref.shape[0]):
        tile = tile + got_ref[p, :, FLAT:]
    flat = iter(unpacked(tile, 21))
    gram = {(i, j): next(flat) for i in range(6) for j in range(i, 6)}
    g00 = symmetric([gram[i, j] for i in range(3) for j in range(i, 3)])
    g01 = [[gram[i, j + 3] for j in range(3)] for i in range(3)]
    g11 = symmetric([gram[i + 3, j + 3] for i in range(3) for j in range(i, 3)])
    n0 = inverse(cholesky(g00))
    n0t = turned(n0)
    c0 = times(times(n0, turned(g01)), n0t)
    l1 = cholesky(minus(times(times(n0, g11), n0t), times(c0, turned(c0))))
    n1 = inverse(l1)
    at = 0
    for matrix in (n0, n1, c0, l1):
        for i in range(3):
            for j in range(3):
                coef_ref[at : at + 1, :] = jnp.broadcast_to(matrix[i][j], (1, 128))
                at += 1


def loaded(coef_ref, which, width):
    row = lambda at: coef_ref[at : at + 1, :]
    wide = lambda v: v if width == 128 else jnp.concatenate([v] * (width // 128), 1)
    return [[wide(row(9 * which + 3 * i + j)) for j in range(3)] for i in range(3)]


def residual_kernel(got_ref, z_ref, x_ref, d_ref, coef_ref, sent_ref, basis_ref):
    total = got_ref[0]
    for p in range(1, got_ref.shape[0]):
        total = total + got_ref[p]
    z = z_ref[...]
    y = rows_of(total + d_ref[...] * z)
    n0, n1, c0, l1 = (loaded(coef_ref, i, W) for i in range(4))
    q0 = combine(n0, rows_of(x_ref[...]))
    u = combine(n0, rows_of(z))
    q1 = combine(n1, [a - b for a, b in zip(u, combine(c0, q0))])
    w = combine(n1, [a - b for a, b in zip(combine(n0, y), combine(c0, u))])
    known = [a + b for a, b in zip(combine(turned(l1), q0), combine(c0, q1))]
    w = [a - b for a, b in zip(w, known)]
    values = [inner(a, b) for a in w for b in q0 + q1]
    values += [inner(w[i], w[j]) for i in range(3) for j in range(i, 3)]
    tile = packed(values)
    for p in range(sent_ref.shape[0]):
        sent_ref[p] = tile
    for at, row in enumerate(q0 + q1 + w):
        basis_ref[at : at + 1, :] = row


def last_kernel(got_ref, basis_ref, coef_ref, out_ref, coeffs_ref):
    tile = got_ref[0]
    for p in range(1, got_ref.shape[0]):
        tile = tile + got_ref[p]
    values = unpacked(tile, 24)
    d0 = [values[6 * i : 6 * i + 3] for i in range(3)]
    d1 = [values[6 * i + 3 : 6 * i + 6] for i in range(3)]
    h2 = minus(minus(symmetric(values[18:]), times(d0, turned(d0))), times(d1, turned(d1)))
    l2 = cholesky(h2)
    n2 = inverse(l2)
    rows = [basis_ref[at : at + 1, :] for at in range(9)]
    q0, q1, w = rows[:3], rows[3:6], rows[6:]
    known = [a + b for a, b in zip(combine(d0, q0), combine(d1, q1))]
    q2 = combine(n2, [a - b for a, b in zip(w, known)])
    root = float(M) ** 0.5
    for k in range(3):
        out_ref[k, 0:1, :] = q1[k] * root
        out_ref[k, 1:2, :] = q2[k] * root
    c0, l1 = ([[v[:, 0:1] for v in line] for line in loaded(coef_ref, i, 128)] for i in (2, 3))
    down = lax.broadcasted_iota(jnp.int32, (3, 3), 0)
    across = lax.broadcasted_iota(jnp.int32, (3, 3), 1)

    def square(matrix, shift):
        tile = jnp.where(down == across, shift, 0.0)
        for i in range(3):
            for j in range(3):
                tile = jnp.where((down == i) & (across == j), tile + matrix[i][j], tile)
        return tile

    second = [[c0[i][j] + d1[i][j] for j in range(3)] for i in range(3)]
    blocks = [[square(c0, SHIFT), square(l1, 0.0)], [square(second, SHIFT), square(l2, 0.0)]]
    for j in range(2):
        for i in range(3):
            for which in range(2):
                coeffs_ref[j, i, which : which + 1, :] = blocks[j][which][i : i + 1, :]


def call(kernel, out, inputs, scratch=(), specs=None, out_specs=None, flops=2_000_000):
    return pl.pallas_call(
        kernel,
        out_shape=out,
        in_specs=specs or [VMEM] * len(inputs),
        out_specs=out_specs or jax.tree.map(lambda _: VMEM, out),
        scratch_shapes=list(scratch),
        cost_estimate=pl.CostEstimate(flops=flops, bytes_accessed=100_000, transcendentals=0),
        name=kernel.__name__,
        compiler_params=pltpu.CompilerParams(vmem_limit_bytes=24 << 20),
    )(*inputs)


def shards(couplings, diag_terms, start_block):
    cols = lax.axis_size("col")
    rows = lax.axis_size("row")
    d = jnp.tile(diag_terms - SHIFT, 3).reshape(1, FLAT)
    swap = [(i, i ^ 1) for i in range(cols)]
    whole = (2 * W, W)
    steps = 2 * W // CHUNK
    f32 = lambda *shape: jax.ShapeDtypeStruct(shape, F32)
    low_scratch = pltpu.VMEM(whole, BF16)
    low_sems = pltpu.SemaphoreType.DMA((3,))

    def stay(array):
        return pltpu.with_memory_space_constraint(array, pltpu.HBM)

    def swapped(block):
        return lax.ppermute(block, "col", swap)

    def collect(got, own, cross):
        sent = call(
            backward_kernel,
            f32(rows, 1, FLAT),
            (got, own, cross, high, stay(low)),
            [low_scratch, pltpu.VMEM((8, 2 * W), F32), low_sems],
            [VMEM] * 4 + [HBM],
        )
        return lax.all_to_all(sent, "row", 0, 0, tiled=True)

    sent, x, high, low = call(
        first_kernel,
        (f32(cols, 1, FLAT), f32(1, FLAT), in_vmem(whole, BF16), pltpu.HBM(whole, BF16)),
        (start_block, stay(couplings)),
        [
            pltpu.VMEM(whole, F32),
            low_scratch,
            pltpu.VMEM((8, W), F32),
            pltpu.VMEM((8, 2 * W), F32),
            pltpu.SemaphoreType.DMA((steps,)),
            pltpu.SemaphoreType.DMA((steps,)),
        ],
        [VMEM, HBM],
        (VMEM, VMEM, VMEM, HBM),
    )
    cross = swapped(x)
    got = lax.all_to_all(sent, "col", 0, 0, tiled=True)
    got = collect(got, x, cross)
    z = jnp.sum(got, axis=0) + d * x
    cross = swapped(z)
    sent = call(
        forward_kernel,
        f32(cols, 1, FLAT + 128),
        (z, x, high, stay(low)),
        [low_scratch, pltpu.VMEM((8, W), F32), pltpu.VMEM((8, 2 * W), F32), low_sems],
        [VMEM] * 3 + [HBM],
    )
    got = lax.all_to_all(sent, "col", 0, 0, tiled=True)
    coef = call(algebra_kernel, f32(40, 128), (got,))
    got = collect(got, z, cross)
    sent, basis = call(residual_kernel, (f32(cols, 1, 128), f32(16, W)), (got, z, x, d, coef))
    got = lax.all_to_all(sent, "col", 0, 0, tiled=True)
    blocks, coeffs = call(last_kernel, (f32(3, 2, W), f32(2, 3, 2, 3)), (got, basis, coef))
    return jnp.swapaxes(blocks, 0, 1), jnp.swapaxes(coeffs, 1, 2)


def solution(mesh):
    placed = (P("row", "col"), P("col"), P(None, "col"))
    return jax.shard_map(
        shards, mesh=mesh, in_specs=placed, out_specs=(P(None, None, "col"), P()), check_vma=False
    )
```

```python
import jax
import jax.numpy as jnp
from jax import lax
from jax.experimental import pallas as pl
from jax.experimental.pallas import tpu as pltpu
from jax.sharding import PartitionSpec as P

M = 24576
SHIFT = 2.5
W = 768
FLAT = 3 * W
CHUNK = 256
F32 = jnp.float32
BF16 = jnp.bfloat16
VMEM = pl.BlockSpec(memory_space=pltpu.VMEM)
HBM = pl.BlockSpec(memory_space=pltpu.HBM)


def in_vmem(shape, dtype=F32):
    return pltpu.VMEM(shape, dtype)


def three_parts(x):
    first = x.astype(BF16).astype(F32)
    rest = x - first
    second = rest.astype(BF16).astype(F32)
    return jnp.concatenate([first, second, rest - second], 0).astype(BF16)


def folded(wide):
    return wide[0:8] + wide[8:16] + wide[16:24]


def over_rows(parts, matrix):
    return lax.dot_general(parts, matrix, (((1,), (1,)), ((), ())), preferred_element_type=F32)


def over_cols(parts, matrix):
    return lax.dot_general(parts, matrix, (((1,), (0,)), ((), ())), preferred_element_type=F32)


def rows_of(flat):
    return [flat[:, k * W : (k + 1) * W] for k in range(3)]


def inner(a, b):
    return jnp.sum(a * b, axis=1, keepdims=True)


def packed(values):
    lane = lax.broadcasted_iota(jnp.int32, (1, 128), 1)
    tile = jnp.zeros((1, 128), F32)
    for at, value in enumerate(values):
        tile = jnp.where(lane == at, value, tile)
    return tile


def unpacked(tile, count):
    lane = lax.broadcasted_iota(jnp.int32, (1, 128), 1)
    return [jnp.sum(jnp.where(lane == at, tile, 0.0), axis=1, keepdims=True) for at in range(count)]


def symmetric(six):
    a, b, c, d, e, f = six
    return [[a, b, c], [b, d, e], [c, e, f]]


def times(a, b):
    return [[sum(a[i][k] * b[k][j] for k in range(3)) for j in range(3)] for i in range(3)]


def turned(a):
    return [[a[j][i] for j in range(3)] for i in range(3)]


def minus(a, b):
    return [[a[i][j] - b[i][j] for j in range(3)] for i in range(3)]


def cholesky(h):
    zero = jnp.zeros_like(h[0][0])
    a = jnp.sqrt(h[0][0])
    b = h[1][0] / a
    c = h[2][0] / a
    d = jnp.sqrt(h[1][1] - b * b)
    e = (h[2][1] - c * b) / d
    f = jnp.sqrt(h[2][2] - c * c - e * e)
    return [[a, zero, zero], [b, d, zero], [c, e, f]]


def inverse(low):
    zero = jnp.zeros_like(low[0][0])
    a, d, f = 1.0 / low[0][0], 1.0 / low[1][1], 1.0 / low[2][2]
    b = -low[1][0] * a * d
    e = -low[2][1] * d * f
    c = -(low[2][0] * a + low[2][1] * b) * f
    return [[a, zero, zero], [b, d, zero], [c, e, f]]


def combine(matrix, vectors):
    return [sum(matrix[i][k] * vectors[k] for k in range(3)) for i in range(3)]


def place(row_index, forward_ref, sent_ref):
    for half in range(2):
        for k in range(3):
            sent_ref[2 * row_index + half, :, k * W : (k + 1) * W] = forward_ref[k : k + 1, half * W : (half + 1) * W]


def first_kernel(x_hbm, d_ref, a_ref, sent_ref, flat_ref, diag_ref, high_ref, low_ref, whole, x_ref, x_rows, forward, sems, x_sem):
    row_index = lax.axis_index("row")
    pieces = [slice(i * CHUNK, (i + 1) * CHUNK) for i in range(2 * W // CHUNK)]
    copies = [pltpu.make_async_copy(a_ref.at[piece], whole.at[piece], sems.at[i]) for i, piece in enumerate(pieces)]
    first = pltpu.make_async_copy(x_hbm, x_ref, x_sem)
    first.start()
    for copy in copies:
        copy.start()
    x_rows[...] = jnp.zeros_like(x_rows)
    first.wait()
    x_rows[0:3, :] = x_ref[...]
    for k in range(3):
        lanes = slice(k * W, (k + 1) * W)
        flat_ref[:, lanes] = x_ref[k : k + 1, :]
        diag_ref[:, lanes] = d_ref[...] - SHIFT
    x = flat_ref[...]
    for p in range(sent_ref.shape[0]):
        sent_ref[p] = x
    parts = three_parts(x_rows[...])
    for copy, piece in zip(copies, pieces):
        copy.wait()
        block = whole[piece, :]
        high = block.astype(BF16)
        low = (block - high.astype(F32)).astype(BF16)
        high_ref[piece, :] = high
        low_ref[piece, :] = low
        forward[:, piece] = 0.5 * folded(over_rows(parts, high) + over_rows(parts, low))
    place(row_index, forward, sent_ref)


def forward_kernel(z_ref, x_ref, high_ref, low_ref, sent_ref, z_rows, forward):
    row_index = lax.axis_index("row")
    z = z_ref[...]
    z_rows[...] = jnp.zeros_like(z_rows)
    for k, row in enumerate(rows_of(z)):
        z_rows[k : k + 1, :] = row
    parts = three_parts(z_rows[...])
    six = rows_of(x_ref[...]) + rows_of(z)
    tile = packed([inner(six[i], six[j]) for i in range(6) for j in range(i, 6)])
    for p in range(sent_ref.shape[0]):
        sent_ref[p, :, 0:FLAT] = z
        sent_ref[p, :, FLAT:] = tile
    forward[...] = 0.5 * folded(over_rows(parts, high_ref[...]) + over_rows(parts, low_ref[...]))
    place(row_index, forward, sent_ref)


def backward_kernel(got_ref, own_ref, cross_ref, high_ref, low_ref, sent_ref, v_rows):
    row_index = lax.axis_index("row")
    col_index = lax.axis_index("col")
    home = col_index // 2 == row_index
    v_rows[...] = jnp.zeros_like(v_rows)
    own = rows_of(own_ref[...])
    cross = rows_of(cross_ref[...]) if cross_ref.shape[0] == 1 else [cross_ref[k : k + 1, :] for k in range(3)]
    for half in range(2):
        sent_here = rows_of(got_ref[2 * row_index + half, :, 0:FLAT])
        for k in range(3):
            mine = jnp.where(col_index % 2 == half, own[k], cross[k])
            v_rows[k : k + 1, half * W : (half + 1) * W] = jnp.where(home, mine, sent_here[k])
    parts = three_parts(v_rows[...])
    total = got_ref[0, :, 0:FLAT]
    for p in range(1, got_ref.shape[0]):
        total = total + got_ref[p, :, 0:FLAT]
    total = rows_of(jnp.where(home, total, 0.0))
    wide = over_cols(parts, high_ref[...]) + over_cols(parts, low_ref[...])
    back = 0.5 * folded(wide)
    for k in range(3):
        part = back[k : k + 1] + total[k]
        for p in range(sent_ref.shape[0]):
            sent_ref[p, :, k * W : (k + 1) * W] = part


def second_backward_kernel(got_ref, own_ref, cross_ref, high_ref, low_ref, sent_ref, coef_ref, v_rows):
    algebra(got_ref, coef_ref)
    backward_kernel(got_ref, own_ref, cross_ref, high_ref, low_ref, sent_ref, v_rows)


def algebra(got_ref, coef_ref):
    tile = got_ref[0, :, FLAT:]
    for p in range(1, got_ref.shape[0]):
        tile = tile + got_ref[p, :, FLAT:]
    flat = iter(unpacked(tile, 21))
    gram = {(i, j): next(flat) for i in range(6) for j in range(i, 6)}
    g00 = symmetric([gram[i, j] for i in range(3) for j in range(i, 3)])
    g01 = [[gram[i, j + 3] for j in range(3)] for i in range(3)]
    g11 = symmetric([gram[i + 3, j + 3] for i in range(3) for j in range(i, 3)])
    n0 = inverse(cholesky(g00))
    n0t = turned(n0)
    c0 = times(times(n0, turned(g01)), n0t)
    l1 = cholesky(minus(times(times(n0, g11), n0t), times(c0, turned(c0))))
    n1 = inverse(l1)
    at = 0
    for matrix in (n0, n1, c0, l1):
        for i in range(3):
            for j in range(3):
                coef_ref[at : at + 1, :] = jnp.broadcast_to(matrix[i][j], (1, 128))
                at += 1


def loaded(coef_ref, which, width):
    row = lambda at: coef_ref[at : at + 1, :]
    wide = lambda v: v if width == 128 else jnp.concatenate([v] * (width // 128), 1)
    return [[wide(row(9 * which + 3 * i + j)) for j in range(3)] for i in range(3)]


def residual_kernel(got_ref, z_ref, x_ref, d_ref, coef_ref, sent_ref, basis_ref):
    total = got_ref[0]
    for p in range(1, got_ref.shape[0]):
        total = total + got_ref[p]
    z = z_ref[...]
    y = rows_of(total + d_ref[...] * z)
    n0, n1, c0, l1 = (loaded(coef_ref, i, W) for i in range(4))
    q0 = combine(n0, rows_of(x_ref[...]))
    u = combine(n0, rows_of(z))
    q1 = combine(n1, [a - b for a, b in zip(u, combine(c0, q0))])
    w = combine(n1, [a - b for a, b in zip(combine(n0, y), combine(c0, u))])
    known = [a + b for a, b in zip(combine(turned(l1), q0), combine(c0, q1))]
    w = [a - b for a, b in zip(w, known)]
    values = [inner(a, b) for a in w for b in q0 + q1]
    values += [inner(w[i], w[j]) for i in range(3) for j in range(i, 3)]
    tile = packed(values)
    for p in range(sent_ref.shape[0]):
        sent_ref[p] = tile
    for at, row in enumerate(q0 + q1 + w):
        basis_ref[at : at + 1, :] = row


def last_kernel(got_ref, basis_ref, coef_ref, out_ref, coeffs_ref):
    tile = got_ref[0]
    for p in range(1, got_ref.shape[0]):
        tile = tile + got_ref[p]
    values = unpacked(tile, 24)
    d0 = [values[6 * i : 6 * i + 3] for i in range(3)]
    d1 = [values[6 * i + 3 : 6 * i + 6] for i in range(3)]
    h2 = minus(minus(symmetric(values[18:]), times(d0, turned(d0))), times(d1, turned(d1)))
    l2 = cholesky(h2)
    n2 = inverse(l2)
    rows = [basis_ref[at : at + 1, :] for at in range(9)]
    q0, q1, w = rows[:3], rows[3:6], rows[6:]
    known = [a + b for a, b in zip(combine(d0, q0), combine(d1, q1))]
    q2 = combine(n2, [a - b for a, b in zip(w, known)])
    root = float(M) ** 0.5
    for k in range(3):
        out_ref[k, 0:1, :] = q1[k] * root
        out_ref[k, 1:2, :] = q2[k] * root
    c0, l1 = ([[v[:, 0:1] for v in line] for line in loaded(coef_ref, i, 128)] for i in (2, 3))
    down = lax.broadcasted_iota(jnp.int32, (3, 3), 0)
    across = lax.broadcasted_iota(jnp.int32, (3, 3), 1)

    def square(matrix, shift):
        tile = jnp.where(down == across, shift, 0.0)
        for i in range(3):
            for j in range(3):
                tile = jnp.where((down == i) & (across == j), tile + matrix[i][j], tile)
        return tile

    second = [[c0[i][j] + d1[i][j] for j in range(3)] for i in range(3)]
    blocks = [[square(c0, SHIFT), square(l1, 0.0)], [square(second, SHIFT), square(l2, 0.0)]]
    for j in range(2):
        for i in range(3):
            for which in range(2):
                coeffs_ref[j, i, which : which + 1, :] = blocks[j][which][i : i + 1, :]


def collect_kernel(got_ref, d_ref, x_ref, z_ref):
    total = got_ref[0]
    for p in range(1, got_ref.shape[0]):
        total = total + got_ref[p]
    z_ref[...] = total + d_ref[...] * x_ref[...]


def call(kernel, out, inputs, scratch=(), specs=None, out_specs=None, flops=2_000_000):
    return pl.pallas_call(
        kernel,
        out_shape=out,
        in_specs=specs or [VMEM] * len(inputs),
        out_specs=out_specs or jax.tree.map(lambda _: VMEM, out),
        scratch_shapes=list(scratch),
        cost_estimate=pl.CostEstimate(flops=flops, bytes_accessed=100_000, transcendentals=0),
        name=kernel.__name__,
        compiler_params=pltpu.CompilerParams(vmem_limit_bytes=24 << 20),
    )(*inputs)


def shards(couplings, diag_terms, start_block):
    cols = lax.axis_size("col")
    rows = lax.axis_size("row")
    swap = [(i, i ^ 1) for i in range(cols)]
    whole = (2 * W, W)
    tall = pltpu.VMEM((8, 2 * W), F32)
    short = pltpu.VMEM((8, W), F32)
    flat = in_vmem((1, FLAT))

    def stay(array):
        return pltpu.with_memory_space_constraint(array, pltpu.HBM)

    def exchanged(block, axis):
        return lax.all_to_all(block, axis, 0, 0, tiled=True)

    cross = lax.ppermute(start_block, "col", swap)
    sent, x, d, high, low = call(
        first_kernel,
        (in_vmem((cols, 1, FLAT)), flat, flat, in_vmem(whole, BF16), in_vmem(whole, BF16)),
        (stay(start_block), diag_terms.reshape(1, W), stay(couplings)),
        [
            pltpu.VMEM(whole, F32),
            pltpu.VMEM((3, W), F32),
            short,
            tall,
            pltpu.SemaphoreType.DMA((2 * W // CHUNK,)),
            pltpu.SemaphoreType.DMA,
        ],
        [HBM, VMEM, HBM],
    )
    sent, cross = lax.optimization_barrier((sent, cross))
    got = exchanged(sent, "col")
    sent = call(backward_kernel, in_vmem((rows, 1, FLAT)), (got, x, cross, high, low), [tall])
    got = exchanged(sent, "row")
    z = call(collect_kernel, flat, (got, d, x))
    cross = lax.ppermute(z, "col", swap)
    sent = call(forward_kernel, in_vmem((cols, 1, FLAT + 128)), (z, x, high, low), [short, tall])
    sent, cross = lax.optimization_barrier((sent, cross))
    got = exchanged(sent, "col")
    sent, coef = call(
        second_backward_kernel,
        (in_vmem((rows, 1, FLAT)), in_vmem((40, 128))),
        (got, z, cross, high, low),
        [tall],
    )
    got = exchanged(sent, "row")
    sent, basis = call(residual_kernel, (in_vmem((cols, 1, 128)), in_vmem((16, W))), (got, z, x, d, coef))
    got = exchanged(sent, "col")
    f32 = lambda *shape: jax.ShapeDtypeStruct(shape, F32)
    blocks, coeffs = call(last_kernel, (f32(3, 2, W), f32(2, 3, 2, 3)), (got, basis, coef))
    return jnp.swapaxes(blocks, 0, 1), jnp.swapaxes(coeffs, 1, 2)


def solution(mesh):
    placed = (P("row", "col"), P("col"), P(None, "col"))
    return jax.shard_map(
        shards, mesh=mesh, in_specs=placed, out_specs=(P(None, None, "col"), P()), check_vma=False
    )
```

```python
import jax
import jax.numpy as jnp
from jax import lax
from jax.experimental import pallas as pl
from jax.experimental.pallas import tpu as pltpu
from jax.sharding import PartitionSpec as P


M = 24576
SHIFT = 2.5
W = 768
FLAT = 3 * W
CHUNK = 256
DEEP = 3
F32 = jnp.float32
BF16 = jnp.bfloat16
VMEM = pl.BlockSpec(memory_space=pltpu.VMEM)
HBM = pl.BlockSpec(memory_space=pltpu.HBM)


def in_vmem(shape, dtype=F32):
    return pltpu.VMEM(shape, dtype)


def three_parts(x):
    first = x.astype(BF16).astype(F32)
    rest = x - first
    second = rest.astype(BF16).astype(F32)
    return jnp.concatenate([first, second, rest - second], 0).astype(BF16)


def folded(wide):
    return wide[0:8] + wide[8:16] + wide[16:24]


def over_rows(parts, matrix):
    return lax.dot_general(parts, matrix, (((1,), (1,)), ((), ())), preferred_element_type=F32)


def over_cols(parts, matrix):
    return lax.dot_general(parts, matrix, (((1,), (0,)), ((), ())), preferred_element_type=F32)


def rows_of(flat):
    return [flat[:, k * W : (k + 1) * W] for k in range(3)]


def inner(a, b):
    return jnp.sum(a * b, axis=1, keepdims=True)


def packed(values):
    lane = lax.broadcasted_iota(jnp.int32, (1, 128), 1)
    tile = jnp.zeros((1, 128), F32)
    for at, value in enumerate(values):
        tile = jnp.where(lane == at, value, tile)
    return tile


def products_of(rows):
    return [sum(inner(a, b) for a, b in zip(rows[i], rows[j])) for i in range(6) for j in range(i, 6)]


def unpacked(tile, count):
    lane = lax.broadcasted_iota(jnp.int32, (1, 128), 1)
    return [jnp.sum(jnp.where(lane == at, tile, 0.0), axis=1, keepdims=True) for at in range(count)]


def symmetric(six):
    a, b, c, d, e, f = six
    return [[a, b, c], [b, d, e], [c, e, f]]


def times(a, b):
    return [[sum(a[i][k] * b[k][j] for k in range(3)) for j in range(3)] for i in range(3)]


def turned(a):
    return [[a[j][i] for j in range(3)] for i in range(3)]


def minus(a, b):
    return [[a[i][j] - b[i][j] for j in range(3)] for i in range(3)]


def cholesky(h):
    zero = jnp.zeros_like(h[0][0])
    a = jnp.sqrt(h[0][0])
    b = h[1][0] / a
    c = h[2][0] / a
    d = jnp.sqrt(h[1][1] - b * b)
    e = (h[2][1] - c * b) / d
    f = jnp.sqrt(h[2][2] - c * c - e * e)
    return [[a, zero, zero], [b, d, zero], [c, e, f]]


def inverse(low):
    zero = jnp.zeros_like(low[0][0])
    a, d, f = 1.0 / low[0][0], 1.0 / low[1][1], 1.0 / low[2][2]
    b = -low[1][0] * a * d
    e = -low[2][1] * d * f
    c = -(low[2][0] * a + low[2][1] * b) * f
    return [[a, zero, zero], [b, d, zero], [c, e, f]]


def combine(matrix, vectors):
    return [sum(matrix[i][k] * vectors[k] for k in range(3)) for i in range(3)]


def place(row_index, forward_ref, sent_ref):
    for half in range(2):
        for k in range(3):
            sent_ref[2 * row_index + half, :, k * W : (k + 1) * W] = forward_ref[k : k + 1, half * W : (half + 1) * W]


def first_kernel(x_hbm, d_hbm, a_ref, sent_ref, flat_ref, diag_ref, high_ref, low_ref, whole, x_ref, d_ref, x_rows, forward, sems, x_sem, d_sem):
    row_index = lax.axis_index("row")
    pieces = [slice(i * CHUNK, (i + 1) * CHUNK) for i in range(2 * W // CHUNK)]
    copies = [pltpu.make_async_copy(a_ref.at[piece], whole.at[piece], sems.at[i]) for i, piece in enumerate(pieces)]
    first = pltpu.make_async_copy(x_hbm, x_ref, x_sem)
    first.start()
    second = pltpu.make_async_copy(d_hbm, d_ref, d_sem)
    second.start()
    for copy in copies[:DEEP]:
        copy.start()
    x_rows[...] = jnp.zeros_like(x_rows)
    first.wait()
    second.wait()
    x_rows[0:3, :] = x_ref[...]
    for k in range(3):
        lanes = slice(k * W, (k + 1) * W)
        flat_ref[:, lanes] = x_ref[k : k + 1, :]
        diag_ref[:, lanes] = d_ref[...].reshape(1, W) - SHIFT
    x = flat_ref[...]
    for p in range(sent_ref.shape[0]):
        sent_ref[p] = x
    parts = three_parts(x_rows[...])
    for i, piece in enumerate(pieces):
        copies[i].wait()
        if i + DEEP < len(copies):
            copies[i + DEEP].start()
        block = whole[piece, :]
        high = block.astype(BF16)
        low = (block - high.astype(F32)).astype(BF16)
        high_ref[piece, :] = high
        low_ref[piece, :] = low
        forward[:, piece] = 0.5 * folded(over_rows(parts, high) + over_rows(parts, low))
    place(row_index, forward, sent_ref)


def forward_kernel(z_ref, x_ref, high_ref, low_ref, sent_ref, z_rows, forward):
    row_index = lax.axis_index("row")
    home = lax.axis_index("col") // 2 == row_index
    z = z_ref[...]
    z_rows[...] = jnp.zeros_like(z_rows)
    for k, row in enumerate(rows_of(z)):
        z_rows[k : k + 1, :] = row
    parts = three_parts(z_rows[...])
    six = rows_of(x_ref[...]) + rows_of(z)
    tile = packed(products_of([[row] for row in six]))
    head = jnp.where(home, z[:, 0:128], tile)
    for p in range(sent_ref.shape[0]):
        sent_ref[p, :, 0:128] = head
        sent_ref[p, :, 128:] = z[:, 128:]
    forward[...] = 0.5 * folded(over_rows(parts, high_ref[...]) + over_rows(parts, low_ref[...]))
    place(row_index, forward, sent_ref)


def first_backward_kernel(got_ref, own_ref, cross_ref, high_ref, low_ref, sent_ref, v_rows):
    backward(got_ref, own_ref, cross_ref, high_ref, low_ref, sent_ref, v_rows)


def second_backward_kernel(got_ref, own_ref, cross_ref, tile_ref, high_ref, low_ref, sent_ref, v_rows):
    for p in range(sent_ref.shape[0]):
        sent_ref[p, :, FLAT:] = tile_ref[...]
    backward(got_ref, own_ref, cross_ref, high_ref, low_ref, sent_ref, v_rows)


def backward(got_ref, own_ref, cross_ref, high_ref, low_ref, sent_ref, v_rows):
    row_index = lax.axis_index("row")
    col_index = lax.axis_index("col")
    home = col_index // 2 == row_index
    v_rows[...] = jnp.zeros_like(v_rows)
    own = rows_of(own_ref[...])
    cross = rows_of(cross_ref[...]) if cross_ref.shape[0] == 1 else [cross_ref[k : k + 1, :] for k in range(3)]
    for half in range(2):
        sent_here = rows_of(got_ref[2 * row_index + half])
        for k in range(3):
            mine = jnp.where(col_index % 2 == half, own[k], cross[k])
            v_rows[k : k + 1, half * W : (half + 1) * W] = jnp.where(home, mine, sent_here[k])
    parts = three_parts(v_rows[...])
    total = got_ref[0]
    for p in range(1, got_ref.shape[0]):
        total = total + got_ref[p]
    total = rows_of(jnp.where(home, total, 0.0))
    wide = over_cols(parts, high_ref[...]) + over_cols(parts, low_ref[...])
    back = 0.5 * folded(wide)
    for k in range(3):
        part = back[k : k + 1] + total[k]
        for p in range(sent_ref.shape[0]):
            sent_ref[p, :, k * W : (k + 1) * W] = part


def gram_kernel(got_ref, x_rows, tile_ref):
    row_index = lax.axis_index("row")
    tile = jnp.zeros((1, 128), F32)
    for p in range(got_ref.shape[0]):
        tile = tile + jnp.where(row_index == p // 2, 0.0, got_ref[p, :, 0:128])
    z = [rows_of(got_ref[2 * row_index + half]) for half in range(2)]
    rows = [[x_rows[k : k + 1, half * W : (half + 1) * W] for half in range(2)] for k in range(3)]
    rows += [[z[half][k] for half in range(2)] for k in range(3)]
    tile_ref[...] = tile + packed(products_of(rows))


def algebra(tile, coef_ref):
    flat = iter(unpacked(tile, 21))
    gram = {(i, j): next(flat) for i in range(6) for j in range(i, 6)}
    g00 = symmetric([gram[i, j] for i in range(3) for j in range(i, 3)])
    g01 = [[gram[i, j + 3] for j in range(3)] for i in range(3)]
    g11 = symmetric([gram[i + 3, j + 3] for i in range(3) for j in range(i, 3)])
    n0 = inverse(cholesky(g00))
    n0t = turned(n0)
    c0 = times(times(n0, turned(g01)), n0t)
    l1 = cholesky(minus(times(times(n0, g11), n0t), times(c0, turned(c0))))
    n1 = inverse(l1)
    at = 0
    for matrix in (n0, n1, c0, l1):
        for i in range(3):
            for j in range(3):
                coef_ref[at : at + 1, :] = jnp.broadcast_to(matrix[i][j], (1, 128))
                at += 1


def loaded(coef_ref, which, width):
    row = lambda at: coef_ref[at : at + 1, :]
    wide = lambda v: v if width == 128 else jnp.concatenate([v] * (width // 128), 1)
    return [[wide(row(9 * which + 3 * i + j)) for j in range(3)] for i in range(3)]


def residual_kernel(got_ref, z_ref, x_ref, d_ref, sent_ref, basis_ref, coef_ref):
    away = (lax.axis_index("col") // 2 + 1) % got_ref.shape[0]
    algebra(got_ref[away, :, FLAT:], coef_ref)
    total = got_ref[0, :, 0:FLAT]
    for p in range(1, got_ref.shape[0]):
        total = total + got_ref[p, :, 0:FLAT]
    z = z_ref[...]
    y = rows_of(total + d_ref[...] * z)
    n0, n1, c0, l1 = (loaded(coef_ref, i, W) for i in range(4))
    q0 = combine(n0, rows_of(x_ref[...]))
    u = combine(n0, rows_of(z))
    q1 = combine(n1, [a - b for a, b in zip(u, combine(c0, q0))])
    w = combine(n1, [a - b for a, b in zip(combine(n0, y), combine(c0, u))])
    known = [a + b for a, b in zip(combine(turned(l1), q0), combine(c0, q1))]
    w = [a - b for a, b in zip(w, known)]
    values = [inner(a, b) for a in w for b in q0 + q1]
    values += [inner(w[i], w[j]) for i in range(3) for j in range(i, 3)]
    tile = packed(values)
    for p in range(sent_ref.shape[0]):
        sent_ref[p] = tile
    for at, row in enumerate(q0 + q1 + w):
        basis_ref[at : at + 1, :] = row


def last_kernel(got_ref, basis_ref, coef_ref, out_ref, coeffs_ref):
    tile = got_ref[0]
    for p in range(1, got_ref.shape[0]):
        tile = tile + got_ref[p]
    values = unpacked(tile, 24)
    d0 = [values[6 * i : 6 * i + 3] for i in range(3)]
    d1 = [values[6 * i + 3 : 6 * i + 6] for i in range(3)]
    h2 = minus(minus(symmetric(values[18:]), times(d0, turned(d0))), times(d1, turned(d1)))
    l2 = cholesky(h2)
    n2 = inverse(l2)
    rows = [basis_ref[at : at + 1, :] for at in range(9)]
    q0, q1, w = rows[:3], rows[3:6], rows[6:]
    known = [a + b for a, b in zip(combine(d0, q0), combine(d1, q1))]
    q2 = combine(n2, [a - b for a, b in zip(w, known)])
    root = float(M) ** 0.5
    for k in range(3):
        out_ref[k, 0:1, :] = q1[k] * root
        out_ref[k, 1:2, :] = q2[k] * root
    c0, l1 = ([[v[:, 0:1] for v in line] for line in loaded(coef_ref, i, 128)] for i in (2, 3))
    down = lax.broadcasted_iota(jnp.int32, (3, 3), 0)
    across = lax.broadcasted_iota(jnp.int32, (3, 3), 1)

    def square(matrix, shift):
        tile = jnp.where(down == across, shift, 0.0)
        for i in range(3):
            for j in range(3):
                tile = jnp.where((down == i) & (across == j), tile + matrix[i][j], tile)
        return tile

    second = [[c0[i][j] + d1[i][j] for j in range(3)] for i in range(3)]
    blocks = [[square(c0, SHIFT), square(l1, 0.0)], [square(second, SHIFT), square(l2, 0.0)]]
    for j in range(2):
        for i in range(3):
            for which in range(2):
                coeffs_ref[j, i, which : which + 1, :] = blocks[j][which][i : i + 1, :]


def collect_kernel(got_ref, d_ref, x_ref, z_ref):
    total = got_ref[0]
    for p in range(1, got_ref.shape[0]):
        total = total + got_ref[p]
    z_ref[...] = total + d_ref[...] * x_ref[...]


def call(kernel, out, inputs, scratch=(), specs=None, out_specs=None, flops=2_000_000):
    return pl.pallas_call(
        kernel,
        out_shape=out,
        in_specs=specs or [VMEM] * len(inputs),
        out_specs=out_specs or jax.tree.map(lambda _: VMEM, out),
        scratch_shapes=list(scratch),
        cost_estimate=pl.CostEstimate(flops=flops, bytes_accessed=100_000, transcendentals=0),
        compiler_params=pltpu.CompilerParams(vmem_limit_bytes=24 << 20),
    )(*inputs)


def shards(couplings, diag_terms, start_block):
    cols = lax.axis_size("col")
    rows = lax.axis_size("row")
    swap = [(i, i ^ 1) for i in range(cols)]
    whole = (2 * W, W)
    tall = pltpu.VMEM((8, 2 * W), F32)
    short = pltpu.VMEM((8, W), F32)
    flat = in_vmem((1, FLAT))

    def stay(array):
        return pltpu.with_memory_space_constraint(array, pltpu.HBM)

    def exchanged(block, axis):
        return lax.all_to_all(block, axis, 0, 0, tiled=True)

    cross = lax.ppermute(start_block, "col", swap)
    sent, x, d, high, low = call(
        first_kernel,
        (in_vmem((cols, 1, FLAT)), flat, flat, in_vmem(whole, BF16), in_vmem(whole, BF16)),
        (stay(start_block), stay(diag_terms), stay(couplings)),
        [
            pltpu.VMEM(whole, F32),
            pltpu.VMEM((3, W), F32),
            pltpu.VMEM((W,), F32),
            short,
            tall,
            pltpu.SemaphoreType.DMA((2 * W // CHUNK,)),
            pltpu.SemaphoreType.DMA,
            pltpu.SemaphoreType.DMA,
        ],
        [HBM, HBM, HBM],
    )
    sent, cross = lax.optimization_barrier((sent, cross))
    got = exchanged(sent, "col")
    many = in_vmem((8, 2 * W))
    sent, x_rows = call(first_backward_kernel, (in_vmem((rows, 1, FLAT)), many), (got, x, cross, high, low))
    got = exchanged(sent, "row")
    z = call(collect_kernel, flat, (got, d, x))
    cross = lax.ppermute(z, "col", swap)
    sent = call(forward_kernel, in_vmem((cols, 1, FLAT)), (z, x, high, low), [short, tall])
    got = exchanged(sent, "col")
    tile = call(gram_kernel, in_vmem((1, 128)), (got, x_rows))
    sent = call(
        second_backward_kernel,
        in_vmem((rows, 1, FLAT + 128)),
        (got, z, cross, tile, high, low),
        [tall],
    )
    got = exchanged(sent, "row")
    sent, basis, coef = call(
        residual_kernel,
        (in_vmem((cols, 1, 128)), in_vmem((16, W)), in_vmem((40, 128))),
        (got, z, x, d),
    )
    got = exchanged(sent, "col")
    f32 = lambda *shape: jax.ShapeDtypeStruct(shape, F32)
    blocks, coeffs = call(last_kernel, (f32(3, 2, W), f32(2, 3, 2, 3)), (got, basis, coef))
    return jnp.swapaxes(blocks, 0, 1), jnp.swapaxes(coeffs, 1, 2)


def solution(mesh):
    placed = (P("row", "col"), P("col"), P(None, "col"))
    return jax.shard_map(
        shards, mesh=mesh, in_specs=placed, out_specs=(P(None, None, "col"), P()), check_vma=False
    )
```

```python
import jax
import jax.numpy as jnp
from jax import lax
from jax.experimental import pallas as pl
from jax.experimental.pallas import tpu as pltpu
from jax.sharding import PartitionSpec as P


M = 24576
SHIFT = 2.5
W = 768
FLAT = 3 * W
CHUNK = 256
DEEP = 3
STRIP = 16
F32 = jnp.float32
BF16 = jnp.bfloat16
VMEM = pl.BlockSpec(memory_space=pltpu.VMEM)
HBM = pl.BlockSpec(memory_space=pltpu.HBM)


def in_vmem(shape, dtype=F32):
    return pltpu.VMEM(shape, dtype)


def three_parts(x):
    first = x.astype(BF16).astype(F32)
    rest = x - first
    second = rest.astype(BF16).astype(F32)
    return jnp.concatenate([first, second, rest - second], 0).astype(BF16)


def folded(wide):
    return wide[0:8] + wide[8:16] + wide[16:24]


def over_rows(parts, matrix):
    return lax.dot_general(parts, matrix, (((1,), (1,)), ((), ())), preferred_element_type=F32)


def over_cols(parts, matrix):
    return lax.dot_general(parts, matrix, (((1,), (0,)), ((), ())), preferred_element_type=F32)


def rows_of(flat):
    return [flat[:, k * W : (k + 1) * W] for k in range(3)]


def inner(a, b):
    return jnp.sum(a * b, axis=1, keepdims=True)


def packed(values):
    lane = lax.broadcasted_iota(jnp.int32, (1, 128), 1)
    tile = jnp.zeros((1, 128), F32)
    for at, value in enumerate(values):
        tile = jnp.where(lane == at, value, tile)
    return tile


def products_of(rows):
    return [sum(inner(a, b) for a, b in zip(rows[i], rows[j])) for i in range(6) for j in range(i, 6)]


def unpacked(tile, count):
    lane = lax.broadcasted_iota(jnp.int32, (1, 128), 1)
    return [jnp.sum(jnp.where(lane == at, tile, 0.0), axis=1, keepdims=True) for at in range(count)]


def symmetric(six):
    a, b, c, d, e, f = six
    return [[a, b, c], [b, d, e], [c, e, f]]


def times(a, b):
    return [[sum(a[i][k] * b[k][j] for k in range(3)) for j in range(3)] for i in range(3)]


def turned(a):
    return [[a[j][i] for j in range(3)] for i in range(3)]


def minus(a, b):
    return [[a[i][j] - b[i][j] for j in range(3)] for i in range(3)]


def cholesky(h):
    zero = jnp.zeros_like(h[0][0])
    a = jnp.sqrt(h[0][0])
    b = h[1][0] / a
    c = h[2][0] / a
    d = jnp.sqrt(h[1][1] - b * b)
    e = (h[2][1] - c * b) / d
    f = jnp.sqrt(h[2][2] - c * c - e * e)
    return [[a, zero, zero], [b, d, zero], [c, e, f]]


def inverse(low):
    zero = jnp.zeros_like(low[0][0])
    a, d, f = 1.0 / low[0][0], 1.0 / low[1][1], 1.0 / low[2][2]
    b = -low[1][0] * a * d
    e = -low[2][1] * d * f
    c = -(low[2][0] * a + low[2][1] * b) * f
    return [[a, zero, zero], [b, d, zero], [c, e, f]]


def combine(matrix, vectors):
    return [sum(matrix[i][k] * vectors[k] for k in range(3)) for i in range(3)]


def place(row_index, forward_ref, sent_ref):
    for half in range(2):
        for k in range(3):
            sent_ref[2 * row_index + half, :, k * W : (k + 1) * W] = forward_ref[k : k + 1, half * W : (half + 1) * W]


def first_kernel(x_hbm, d_hbm, a_ref, sent_ref, flat_ref, diag_ref, high_ref, low_ref, whole, x_ref, d_ref, x_rows, forward, sems, x_sem, d_sem):
    row_index = lax.axis_index("row")
    pieces = [slice(i * CHUNK, (i + 1) * CHUNK) for i in range(2 * W // CHUNK)]
    copies = [pltpu.make_async_copy(a_ref.at[piece], whole.at[piece], sems.at[i]) for i, piece in enumerate(pieces)]
    first = pltpu.make_async_copy(x_hbm, x_ref, x_sem)
    first.start()
    second = pltpu.make_async_copy(d_hbm, d_ref, d_sem)
    second.start()
    for copy in copies[:DEEP]:
        copy.start()
    x_rows[...] = jnp.zeros_like(x_rows)
    first.wait()
    second.wait()
    x_rows[0:3, :] = x_ref[...]
    for k in range(3):
        lanes = slice(k * W, (k + 1) * W)
        flat_ref[:, lanes] = x_ref[k : k + 1, :]
        diag_ref[:, lanes] = d_ref[...].reshape(1, W) - SHIFT
    x = flat_ref[...]
    for p in range(sent_ref.shape[0]):
        sent_ref[p] = x
    parts = three_parts(x_rows[...])
    for i in range(len(pieces) + 1):
        if i < len(pieces):
            piece = pieces[i]
            copies[i].wait()
            if i + DEEP < len(copies):
                copies[i + DEEP].start()
            for at in range(i * CHUNK, (i + 1) * CHUNK, STRIP):
                strip = slice(at, at + STRIP)
                block = whole[strip, :]
                high = block.astype(BF16)
                high_ref[strip, :] = high
                low_ref[strip, :] = (block - high.astype(F32)).astype(BF16)
        if i > 0:
            piece = pieces[i - 1]
            wide = over_rows(parts, high_ref[piece, :]) + over_rows(parts, low_ref[piece, :])
            forward[:, piece] = 0.5 * folded(wide)
    place(row_index, forward, sent_ref)


def forward_kernel(z_ref, x_ref, high_ref, low_ref, sent_ref, z_rows, forward):
    row_index = lax.axis_index("row")
    home = lax.axis_index("col") // 2 == row_index
    z = z_ref[...]
    z_rows[...] = jnp.zeros_like(z_rows)
    for k, row in enumerate(rows_of(z)):
        z_rows[k : k + 1, :] = row
    parts = three_parts(z_rows[...])
    six = rows_of(x_ref[...]) + rows_of(z)
    tile = packed(products_of([[row] for row in six]))
    head = jnp.where(home, z[:, 0:128], tile)
    for p in range(sent_ref.shape[0]):
        sent_ref[p, :, 0:128] = head
        sent_ref[p, :, 128:] = z[:, 128:]
    forward[...] = 0.5 * folded(over_rows(parts, high_ref[...]) + over_rows(parts, low_ref[...]))
    place(row_index, forward, sent_ref)


def first_backward_kernel(got_ref, own_ref, cross_ref, total_ref, high_ref, low_ref, sent_ref, v_rows):
    backward(got_ref, own_ref, cross_ref, total_ref, high_ref, low_ref, sent_ref, v_rows)


def second_backward_kernel(got_ref, own_ref, cross_ref, total_ref, tile_ref, high_ref, low_ref, sent_ref, v_rows):
    for p in range(sent_ref.shape[0]):
        sent_ref[p, :, FLAT:] = tile_ref[...]
    backward(got_ref, own_ref, cross_ref, total_ref, high_ref, low_ref, sent_ref, v_rows)


def backward(got_ref, own_ref, cross_ref, total_ref, high_ref, low_ref, sent_ref, v_rows):
    row_index = lax.axis_index("row")
    col_index = lax.axis_index("col")
    home = col_index // 2 == row_index
    v_rows[...] = jnp.zeros_like(v_rows)
    own = rows_of(own_ref[...])
    cross = rows_of(cross_ref[...])
    for half in range(2):
        sent_here = rows_of(got_ref[2 * row_index + half])
        for k in range(3):
            mine = jnp.where(col_index % 2 == half, own[k], cross[k])
            v_rows[k : k + 1, half * W : (half + 1) * W] = jnp.where(home, mine, sent_here[k])
    parts = three_parts(v_rows[...])
    total = rows_of(total_ref[...])
    wide = over_cols(parts, high_ref[...]) + over_cols(parts, low_ref[...])
    back = 0.5 * folded(wide)
    for k in range(3):
        part = back[k : k + 1] + total[k]
        for p in range(sent_ref.shape[0]):
            sent_ref[p, :, k * W : (k + 1) * W] = part


def sum_kernel(got_ref, total_ref):
    home = lax.axis_index("col") // 2 == lax.axis_index("row")
    total = got_ref[0]
    for p in range(1, got_ref.shape[0]):
        total = total + got_ref[p]
    total_ref[...] = jnp.where(home, total, 0.0)


def gram_kernel(got_ref, x_rows, total_ref, tile_ref):
    sum_kernel(got_ref, total_ref)
    row_index = lax.axis_index("row")
    tile = jnp.zeros((1, 128), F32)
    for p in range(got_ref.shape[0]):
        tile = tile + jnp.where(row_index == p // 2, 0.0, got_ref[p, :, 0:128])
    z = [rows_of(got_ref[2 * row_index + half]) for half in range(2)]
    rows = [[x_rows[k : k + 1, half * W : (half + 1) * W] for half in range(2)] for k in range(3)]
    rows += [[z[half][k] for half in range(2)] for k in range(3)]
    tile_ref[...] = tile + packed(products_of(rows))


def algebra(tile, coef_ref):
    flat = iter(unpacked(tile, 21))
    gram = {(i, j): next(flat) for i in range(6) for j in range(i, 6)}
    g00 = symmetric([gram[i, j] for i in range(3) for j in range(i, 3)])
    g01 = [[gram[i, j + 3] for j in range(3)] for i in range(3)]
    g11 = symmetric([gram[i + 3, j + 3] for i in range(3) for j in range(i, 3)])
    n0 = inverse(cholesky(g00))
    n0t = turned(n0)
    c0 = times(times(n0, turned(g01)), n0t)
    l1 = cholesky(minus(times(times(n0, g11), n0t), times(c0, turned(c0))))
    n1 = inverse(l1)
    at = 0
    for matrix in (n0, n1, c0, l1):
        for i in range(3):
            for j in range(3):
                coef_ref[at : at + 1, :] = jnp.broadcast_to(matrix[i][j], (1, 128))
                at += 1


def loaded(coef_ref, which, width):
    row = lambda at: coef_ref[at : at + 1, :]
    wide = lambda v: v if width == 128 else jnp.concatenate([v] * (width // 128), 1)
    return [[wide(row(9 * which + 3 * i + j)) for j in range(3)] for i in range(3)]


def residual_kernel(got_ref, z_ref, x_ref, d_ref, sent_ref, basis_ref, coef_ref):
    away = (lax.axis_index("col") // 2 + 1) % got_ref.shape[0]
    algebra(got_ref[away, :, FLAT:], coef_ref)
    total = got_ref[0, :, 0:FLAT]
    for p in range(1, got_ref.shape[0]):
        total = total + got_ref[p, :, 0:FLAT]
    z = z_ref[...]
    y = rows_of(total + d_ref[...] * z)
    n0, n1, c0, l1 = (loaded(coef_ref, i, W) for i in range(4))
    q0 = combine(n0, rows_of(x_ref[...]))
    u = combine(n0, rows_of(z))
    q1 = combine(n1, [a - b for a, b in zip(u, combine(c0, q0))])
    w = combine(n1, [a - b for a, b in zip(combine(n0, y), combine(c0, u))])
    known = [a + b for a, b in zip(combine(turned(l1), q0), combine(c0, q1))]
    w = [a - b for a, b in zip(w, known)]
    values = [inner(a, b) for a in w for b in q0 + q1]
    values += [inner(w[i], w[j]) for i in range(3) for j in range(i, 3)]
    tile = packed(values)
    for p in range(sent_ref.shape[0]):
        sent_ref[p] = tile
    for at, row in enumerate(q0 + q1 + w):
        basis_ref[at : at + 1, :] = row


def last_kernel(got_ref, basis_ref, coef_ref, out_ref, coeffs_ref):
    tile = got_ref[0]
    for p in range(1, got_ref.shape[0]):
        tile = tile + got_ref[p]
    values = unpacked(tile, 24)
    d0 = [values[6 * i : 6 * i + 3] for i in range(3)]
    d1 = [values[6 * i + 3 : 6 * i + 6] for i in range(3)]
    h2 = minus(minus(symmetric(values[18:]), times(d0, turned(d0))), times(d1, turned(d1)))
    l2 = cholesky(h2)
    n2 = inverse(l2)
    rows = [basis_ref[at : at + 1, :] for at in range(9)]
    q0, q1, w = rows[:3], rows[3:6], rows[6:]
    known = [a + b for a, b in zip(combine(d0, q0), combine(d1, q1))]
    q2 = combine(n2, [a - b for a, b in zip(w, known)])
    root = float(M) ** 0.5
    for k in range(3):
        out_ref[k, 0:1, :] = q1[k] * root
        out_ref[k, 1:2, :] = q2[k] * root
    c0, l1 = ([[v[:, 0:1] for v in line] for line in loaded(coef_ref, i, 128)] for i in (2, 3))
    down = lax.broadcasted_iota(jnp.int32, (3, 3), 0)
    across = lax.broadcasted_iota(jnp.int32, (3, 3), 1)

    def square(matrix, shift):
        tile = jnp.where(down == across, shift, 0.0)
        for i in range(3):
            for j in range(3):
                tile = jnp.where((down == i) & (across == j), tile + matrix[i][j], tile)
        return tile

    second = [[c0[i][j] + d1[i][j] for j in range(3)] for i in range(3)]
    blocks = [[square(c0, SHIFT), square(l1, 0.0)], [square(second, SHIFT), square(l2, 0.0)]]
    for j in range(2):
        for i in range(3):
            for which in range(2):
                coeffs_ref[j, i, which : which + 1, :] = blocks[j][which][i : i + 1, :]


def collect_kernel(got_ref, d_ref, x_ref, z_ref):
    total = got_ref[0]
    for p in range(1, got_ref.shape[0]):
        total = total + got_ref[p]
    z_ref[...] = total + d_ref[...] * x_ref[...]


def call(kernel, out, inputs, scratch=(), specs=None, out_specs=None, flops=2_000_000):
    return pl.pallas_call(
        kernel,
        out_shape=out,
        in_specs=specs or [VMEM] * len(inputs),
        out_specs=out_specs or jax.tree.map(lambda _: VMEM, out),
        scratch_shapes=list(scratch),
        cost_estimate=pl.CostEstimate(flops=flops, bytes_accessed=100_000, transcendentals=0),
        compiler_params=pltpu.CompilerParams(vmem_limit_bytes=24 << 20),
    )(*inputs)


def shards(couplings, diag_terms, start_block):
    cols = lax.axis_size("col")
    rows = lax.axis_size("row")
    swap = [(i, i ^ 1) for i in range(cols)]
    whole = (2 * W, W)
    tall = pltpu.VMEM((8, 2 * W), F32)
    short = pltpu.VMEM((8, W), F32)
    flat = in_vmem((1, FLAT))

    def stay(array):
        return pltpu.with_memory_space_constraint(array, pltpu.HBM)

    def exchanged(block, axis):
        return lax.all_to_all(block, axis, 0, 0, tiled=True)

    def spread(sent, block):
        cross = lax.ppermute(block, "col", swap)
        return exchanged(sent, "col"), cross

    sent, x, d, high, low = call(
        first_kernel,
        (in_vmem((cols, 1, FLAT)), flat, flat, in_vmem(whole, BF16), in_vmem(whole, BF16)),
        (stay(start_block), stay(diag_terms), stay(couplings)),
        [
            pltpu.VMEM(whole, F32),
            pltpu.VMEM((3, W), F32),
            pltpu.VMEM((W,), F32),
            short,
            tall,
            pltpu.SemaphoreType.DMA((2 * W // CHUNK,)),
            pltpu.SemaphoreType.DMA,
            pltpu.SemaphoreType.DMA,
        ],
        [HBM, HBM, HBM],
    )
    got, cross = spread(sent, x)
    total = call(sum_kernel, flat, (got,))
    many = in_vmem((8, 2 * W))
    sent, x_rows = call(
        first_backward_kernel, (in_vmem((rows, 1, FLAT)), many), (got, x, cross, total, high, low)
    )
    got = exchanged(sent, "row")
    z = call(collect_kernel, flat, (got, d, x))
    sent = call(forward_kernel, in_vmem((cols, 1, FLAT)), (z, x, high, low), [short, tall])
    got, cross = spread(sent, z)
    total, tile = call(gram_kernel, (flat, in_vmem((1, 128))), (got, x_rows))
    sent = call(
        second_backward_kernel,
        in_vmem((rows, 1, FLAT + 128)),
        (got, z, cross, total, tile, high, low),
        [tall],
    )
    got = exchanged(sent, "row")
    sent, basis, coef = call(
        residual_kernel,
        (in_vmem((cols, 1, 128)), in_vmem((16, W)), in_vmem((40, 128))),
        (got, z, x, d),
    )
    got = exchanged(sent, "col")
    f32 = lambda *shape: jax.ShapeDtypeStruct(shape, F32)
    blocks, coeffs = call(last_kernel, (f32(3, 2, W), f32(2, 3, 2, 3)), (got, basis, coef))
    return jnp.swapaxes(blocks, 0, 1), jnp.swapaxes(coeffs, 1, 2)


def solution(mesh):
    placed = (P("row", "col"), P("col"), P(None, "col"))
    return jax.shard_map(
        shards, mesh=mesh, in_specs=placed, out_specs=(P(None, None, "col"), P()), check_vma=False
    )
```

```python
import jax
import jax.numpy as jnp
from jax import lax
from jax.experimental import pallas as pl
from jax.experimental.pallas import tpu as pltpu
from jax.sharding import PartitionSpec as P


M = 24576
SHIFT = 2.5
W = 768
FLAT = 3 * W
CHUNK = 512
STRIP = 16
F32 = jnp.float32
BF16 = jnp.bfloat16
VMEM = pl.BlockSpec(memory_space=pltpu.VMEM)
HBM = pl.BlockSpec(memory_space=pltpu.HBM)


def in_vmem(shape, dtype=F32):
    return pltpu.VMEM(shape, dtype)


def three_parts(x):
    first = x.astype(BF16).astype(F32)
    rest = x - first
    second = rest.astype(BF16).astype(F32)
    return jnp.concatenate([first, second, rest - second], 0).astype(BF16)


def folded(wide):
    return wide[0:8] + wide[8:16] + wide[16:24]


def over_rows(parts, matrix):
    return lax.dot_general(parts, matrix, (((1,), (1,)), ((), ())), preferred_element_type=F32)


def over_cols(parts, matrix):
    return lax.dot_general(parts, matrix, (((1,), (0,)), ((), ())), preferred_element_type=F32)


def rows_of(flat):
    return [flat[:, k * W : (k + 1) * W] for k in range(3)]


def inner(a, b):
    return jnp.sum(a * b, axis=1, keepdims=True)


def packed(values):
    lane = lax.broadcasted_iota(jnp.int32, (1, 128), 1)
    tile = jnp.zeros((1, 128), F32)
    for at, value in enumerate(values):
        tile = jnp.where(lane == at, value, tile)
    return tile


def products_of(rows):
    return [sum(inner(a, b) for a, b in zip(rows[i], rows[j])) for i in range(6) for j in range(i, 6)]


def unpacked(tile, count):
    lane = lax.broadcasted_iota(jnp.int32, (1, 128), 1)
    return [jnp.sum(jnp.where(lane == at, tile, 0.0), axis=1, keepdims=True) for at in range(count)]


def symmetric(six):
    a, b, c, d, e, f = six
    return [[a, b, c], [b, d, e], [c, e, f]]


def times(a, b):
    return [[sum(a[i][k] * b[k][j] for k in range(3)) for j in range(3)] for i in range(3)]


def turned(a):
    return [[a[j][i] for j in range(3)] for i in range(3)]


def minus(a, b):
    return [[a[i][j] - b[i][j] for j in range(3)] for i in range(3)]


def cholesky(h):
    zero = jnp.zeros_like(h[0][0])
    a = jnp.sqrt(h[0][0])
    b = h[1][0] / a
    c = h[2][0] / a
    d = jnp.sqrt(h[1][1] - b * b)
    e = (h[2][1] - c * b) / d
    f = jnp.sqrt(h[2][2] - c * c - e * e)
    return [[a, zero, zero], [b, d, zero], [c, e, f]]


def inverse(low):
    zero = jnp.zeros_like(low[0][0])
    a, d, f = 1.0 / low[0][0], 1.0 / low[1][1], 1.0 / low[2][2]
    b = -low[1][0] * a * d
    e = -low[2][1] * d * f
    c = -(low[2][0] * a + low[2][1] * b) * f
    return [[a, zero, zero], [b, d, zero], [c, e, f]]


def combine(matrix, vectors):
    return [sum(matrix[i][k] * vectors[k] for k in range(3)) for i in range(3)]


def place(row_index, forward_ref, sent_ref):
    for half in range(2):
        for k in range(3):
            sent_ref[2 * row_index + half, :, k * W : (k + 1) * W] = forward_ref[k : k + 1, half * W : (half + 1) * W]


def prepare_kernel(x_hbm, d_hbm, flat_ref, diag_ref, rows_ref, x_ref, d_ref, x_sem, d_sem):
    first = pltpu.make_async_copy(x_hbm, x_ref, x_sem)
    second = pltpu.make_async_copy(d_hbm, d_ref, d_sem)
    first.start()
    second.start()
    rows_ref[...] = jnp.zeros_like(rows_ref)
    first.wait()
    second.wait()
    rows_ref[0:3, :] = x_ref[...]
    for k in range(3):
        lanes = slice(k * W, (k + 1) * W)
        flat_ref[:, lanes] = x_ref[k : k + 1, :]
        diag_ref[:, lanes] = d_ref[...].reshape(1, W) - SHIFT


def first_kernel(x_ref, rows_ref, a_ref, sent_ref, high_ref, low_ref, forward):
    row_index = lax.axis_index("row")
    x = x_ref[...]
    for p in range(sent_ref.shape[0]):
        sent_ref[p] = x
    parts = three_parts(rows_ref[...])
    for start in range(0, 2 * W, CHUNK):
        piece = slice(start, start + CHUNK)
        for at in range(start, start + CHUNK, STRIP):
            strip = slice(at, at + STRIP)
            block = a_ref[strip, :]
            high = block.astype(BF16)
            high_ref[strip, :] = high
            low_ref[strip, :] = (block - high.astype(F32)).astype(BF16)
        wide = over_rows(parts, high_ref[piece, :]) + over_rows(parts, low_ref[piece, :])
        forward[:, piece] = 0.5 * folded(wide)
    place(row_index, forward, sent_ref)


def forward_kernel(z_ref, x_ref, high_ref, low_ref, sent_ref, z_rows, forward):
    row_index = lax.axis_index("row")
    home = lax.axis_index("col") // 2 == row_index
    z = z_ref[...]
    z_rows[...] = jnp.zeros_like(z_rows)
    for k, row in enumerate(rows_of(z)):
        z_rows[k : k + 1, :] = row
    parts = three_parts(z_rows[...])
    six = rows_of(x_ref[...]) + rows_of(z)
    tile = packed(products_of([[row] for row in six]))
    head = jnp.where(home, z[:, 0:128], tile)
    for p in range(sent_ref.shape[0]):
        sent_ref[p, :, 0:128] = head
        sent_ref[p, :, 128:] = z[:, 128:]
    forward[...] = 0.5 * folded(over_rows(parts, high_ref[...]) + over_rows(parts, low_ref[...]))
    place(row_index, forward, sent_ref)


def first_backward_kernel(got_ref, own_ref, cross_ref, total_ref, high_ref, low_ref, sent_ref, v_rows):
    backward(got_ref, own_ref, cross_ref, total_ref, high_ref, low_ref, sent_ref, v_rows)


def second_backward_kernel(got_ref, own_ref, cross_ref, total_ref, tile_ref, high_ref, low_ref, sent_ref, v_rows):
    for p in range(sent_ref.shape[0]):
        sent_ref[p, :, FLAT:] = tile_ref[...]
    backward(got_ref, own_ref, cross_ref, total_ref, high_ref, low_ref, sent_ref, v_rows)


def backward(got_ref, own_ref, cross_ref, total_ref, high_ref, low_ref, sent_ref, v_rows):
    row_index = lax.axis_index("row")
    col_index = lax.axis_index("col")
    home = col_index // 2 == row_index
    v_rows[...] = jnp.zeros_like(v_rows)
    own = rows_of(own_ref[...])
    cross = rows_of(cross_ref[...])
    for half in range(2):
        sent_here = rows_of(got_ref[2 * row_index + half])
        for k in range(3):
            mine = jnp.where(col_index % 2 == half, own[k], cross[k])
            v_rows[k : k + 1, half * W : (half + 1) * W] = jnp.where(home, mine, sent_here[k])
    parts = three_parts(v_rows[...])
    total = rows_of(total_ref[...])
    wide = over_cols(parts, high_ref[...]) + over_cols(parts, low_ref[...])
    back = 0.5 * folded(wide)
    for k in range(3):
        part = back[k : k + 1] + total[k]
        for p in range(sent_ref.shape[0]):
            sent_ref[p, :, k * W : (k + 1) * W] = part


def sum_kernel(got_ref, total_ref):
    home = lax.axis_index("col") // 2 == lax.axis_index("row")
    total = got_ref[0]
    for p in range(1, got_ref.shape[0]):
        total = total + got_ref[p]
    total_ref[...] = jnp.where(home, total, 0.0)


def gram_kernel(got_ref, x_rows, total_ref, tile_ref):
    sum_kernel(got_ref, total_ref)
    row_index = lax.axis_index("row")
    tile = jnp.zeros((1, 128), F32)
    for p in range(got_ref.shape[0]):
        tile = tile + jnp.where(row_index == p // 2, 0.0, got_ref[p, :, 0:128])
    z = [rows_of(got_ref[2 * row_index + half]) for half in range(2)]
    rows = [[x_rows[k : k + 1, half * W : (half + 1) * W] for half in range(2)] for k in range(3)]
    rows += [[z[half][k] for half in range(2)] for k in range(3)]
    tile_ref[...] = tile + packed(products_of(rows))


def algebra(tile, coef_ref):
    flat = iter(unpacked(tile, 21))
    gram = {(i, j): next(flat) for i in range(6) for j in range(i, 6)}
    g00 = symmetric([gram[i, j] for i in range(3) for j in range(i, 3)])
    g01 = [[gram[i, j + 3] for j in range(3)] for i in range(3)]
    g11 = symmetric([gram[i + 3, j + 3] for i in range(3) for j in range(i, 3)])
    n0 = inverse(cholesky(g00))
    n0t = turned(n0)
    c0 = times(times(n0, turned(g01)), n0t)
    l1 = cholesky(minus(times(times(n0, g11), n0t), times(c0, turned(c0))))
    n1 = inverse(l1)
    at = 0
    for matrix in (n0, n1, c0, l1):
        for i in range(3):
            for j in range(3):
                coef_ref[at : at + 1, :] = jnp.broadcast_to(matrix[i][j], (1, 128))
                at += 1


def loaded(coef_ref, which, width):
    row = lambda at: coef_ref[at : at + 1, :]
    wide = lambda v: v if width == 128 else jnp.concatenate([v] * (width // 128), 1)
    return [[wide(row(9 * which + 3 * i + j)) for j in range(3)] for i in range(3)]


def residual_kernel(got_ref, z_ref, x_ref, d_ref, sent_ref, basis_ref, coef_ref):
    away = (lax.axis_index("col") // 2 + 1) % got_ref.shape[0]
    algebra(got_ref[away, :, FLAT:], coef_ref)
    total = got_ref[0, :, 0:FLAT]
    for p in range(1, got_ref.shape[0]):
        total = total + got_ref[p, :, 0:FLAT]
    z = z_ref[...]
    y = rows_of(total + d_ref[...] * z)
    n0, n1, c0, l1 = (loaded(coef_ref, i, W) for i in range(4))
    q0 = combine(n0, rows_of(x_ref[...]))
    u = combine(n0, rows_of(z))
    q1 = combine(n1, [a - b for a, b in zip(u, combine(c0, q0))])
    w = combine(n1, [a - b for a, b in zip(combine(n0, y), combine(c0, u))])
    known = [a + b for a, b in zip(combine(turned(l1), q0), combine(c0, q1))]
    w = [a - b for a, b in zip(w, known)]
    values = [inner(a, b) for a in w for b in q0 + q1]
    values += [inner(w[i], w[j]) for i in range(3) for j in range(i, 3)]
    tile = packed(values)
    for p in range(sent_ref.shape[0]):
        sent_ref[p] = tile
    for at, row in enumerate(q0 + q1 + w):
        basis_ref[at : at + 1, :] = row


def last_kernel(got_ref, basis_ref, coef_ref, out_ref, coeffs_ref):
    tile = got_ref[0]
    for p in range(1, got_ref.shape[0]):
        tile = tile + got_ref[p]
    values = unpacked(tile, 24)
    d0 = [values[6 * i : 6 * i + 3] for i in range(3)]
    d1 = [values[6 * i + 3 : 6 * i + 6] for i in range(3)]
    h2 = minus(minus(symmetric(values[18:]), times(d0, turned(d0))), times(d1, turned(d1)))
    l2 = cholesky(h2)
    n2 = inverse(l2)
    rows = [basis_ref[at : at + 1, :] for at in range(9)]
    q0, q1, w = rows[:3], rows[3:6], rows[6:]
    known = [a + b for a, b in zip(combine(d0, q0), combine(d1, q1))]
    q2 = combine(n2, [a - b for a, b in zip(w, known)])
    root = float(M) ** 0.5
    for k in range(3):
        out_ref[k, 0:1, :] = q1[k] * root
        out_ref[k, 1:2, :] = q2[k] * root
    c0, l1 = ([[v[:, 0:1] for v in line] for line in loaded(coef_ref, i, 128)] for i in (2, 3))
    down = lax.broadcasted_iota(jnp.int32, (3, 3), 0)
    across = lax.broadcasted_iota(jnp.int32, (3, 3), 1)

    def square(matrix, shift):
        tile = jnp.where(down == across, shift, 0.0)
        for i in range(3):
            for j in range(3):
                tile = jnp.where((down == i) & (across == j), tile + matrix[i][j], tile)
        return tile

    second = [[c0[i][j] + d1[i][j] for j in range(3)] for i in range(3)]
    blocks = [[square(c0, SHIFT), square(l1, 0.0)], [square(second, SHIFT), square(l2, 0.0)]]
    for j in range(2):
        for i in range(3):
            for which in range(2):
                coeffs_ref[j, i, which : which + 1, :] = blocks[j][which][i : i + 1, :]


def collect_kernel(got_ref, d_ref, x_ref, z_ref):
    total = got_ref[0]
    for p in range(1, got_ref.shape[0]):
        total = total + got_ref[p]
    z_ref[...] = total + d_ref[...] * x_ref[...]


def call(kernel, out, inputs, scratch=(), specs=None, out_specs=None, flops=2_000_000):
    return pl.pallas_call(
        kernel,
        out_shape=out,
        in_specs=specs or [VMEM] * len(inputs),
        out_specs=out_specs or jax.tree.map(lambda _: VMEM, out),
        scratch_shapes=list(scratch),
        cost_estimate=pl.CostEstimate(flops=flops, bytes_accessed=100_000, transcendentals=0),
        compiler_params=pltpu.CompilerParams(vmem_limit_bytes=24 << 20),
    )(*inputs)


def shards(couplings, diag_terms, start_block):
    cols = lax.axis_size("col")
    rows = lax.axis_size("row")
    swap = [(i, i ^ 1) for i in range(cols)]
    whole = (2 * W, W)
    tall = pltpu.VMEM((8, 2 * W), F32)
    short = pltpu.VMEM((8, W), F32)
    flat = in_vmem((1, FLAT))

    def stay(array):
        return pltpu.with_memory_space_constraint(array, pltpu.HBM)

    def exchanged(block, axis):
        return lax.all_to_all(block, axis, 0, 0, tiled=True)

    def spread(sent, block):
        cross = lax.ppermute(block, "col", swap)
        return exchanged(sent, "col"), cross

    x, d, x_eight = call(
        prepare_kernel,
        (flat, flat, in_vmem((8, W))),
        (stay(start_block), stay(diag_terms)),
        [pltpu.VMEM((3, W), F32), pltpu.VMEM((W,), F32), pltpu.SemaphoreType.DMA, pltpu.SemaphoreType.DMA],
        [HBM, HBM],
        flops=5_000_000_000,
    )
    cross = lax.ppermute(x, "col", swap)
    sent, high, low = call(
        first_kernel,
        (in_vmem((cols, 1, FLAT)), in_vmem(whole, BF16), in_vmem(whole, BF16)),
        (x, x_eight, couplings),
        [tall],
    )
    got = exchanged(sent, "col")
    total = call(sum_kernel, flat, (got,))
    many = in_vmem((8, 2 * W))
    sent, x_rows = call(
        first_backward_kernel, (in_vmem((rows, 1, FLAT)), many), (got, x, cross, total, high, low)
    )
    got = exchanged(sent, "row")
    z = call(collect_kernel, flat, (got, d, x))
    sent = call(forward_kernel, in_vmem((cols, 1, FLAT)), (z, x, high, low), [short, tall])
    got, cross = spread(sent, z)
    total, tile = call(gram_kernel, (flat, in_vmem((1, 128))), (got, x_rows))
    sent = call(
        second_backward_kernel,
        in_vmem((rows, 1, FLAT + 128)),
        (got, z, cross, total, tile, high, low),
        [tall],
    )
    got = exchanged(sent, "row")
    sent, basis, coef = call(
        residual_kernel,
        (in_vmem((cols, 1, 128)), in_vmem((16, W)), in_vmem((40, 128))),
        (got, z, x, d),
    )
    got = exchanged(sent, "col")
    f32 = lambda *shape: jax.ShapeDtypeStruct(shape, F32)
    blocks, coeffs = call(last_kernel, (f32(3, 2, W), f32(2, 3, 2, 3)), (got, basis, coef))
    return jnp.swapaxes(blocks, 0, 1), jnp.swapaxes(coeffs, 1, 2)


def solution(mesh):
    placed = (P("row", "col"), P("col"), P(None, "col"))
    return jax.shard_map(
        shards, mesh=mesh, in_specs=placed, out_specs=(P(None, None, "col"), P()), check_vma=False
    )
```

```python
import jax
import jax.numpy as jnp
from jax import lax
from jax.experimental import pallas as pl
from jax.experimental.pallas import tpu as pltpu
from jax.sharding import PartitionSpec as P


M = 24576
SHIFT = 2.5
W = 768
FLAT = 3 * W
CHUNK = 512
STRIP = 16
F32 = jnp.float32
BF16 = jnp.bfloat16
VMEM = pl.BlockSpec(memory_space=pltpu.VMEM)


def in_vmem(shape, dtype=F32):
    return pltpu.VMEM(shape, dtype)


def three_parts(x):
    first = x.astype(BF16).astype(F32)
    rest = x - first
    second = rest.astype(BF16).astype(F32)
    return jnp.concatenate([first, second, rest - second], 0).astype(BF16)


def folded(wide):
    return wide[0:8] + wide[8:16] + wide[16:24]


def over_rows(parts, matrix):
    return lax.dot_general(parts, matrix, (((1,), (1,)), ((), ())), preferred_element_type=F32)


def over_cols(parts, matrix):
    return lax.dot_general(parts, matrix, (((1,), (0,)), ((), ())), preferred_element_type=F32)


def rows_of(flat):
    return [flat[:, k * W : (k + 1) * W] for k in range(3)]


def inner(a, b):
    return jnp.sum(a * b, axis=1, keepdims=True)


def packed(values):
    lane = lax.broadcasted_iota(jnp.int32, (1, 128), 1)
    tile = jnp.zeros((1, 128), F32)
    for at, value in enumerate(values):
        tile = jnp.where(lane == at, value, tile)
    return tile


def products_of(rows):
    return [sum(inner(a, b) for a, b in zip(rows[i], rows[j])) for i in range(6) for j in range(i, 6)]


def unpacked(tile, count):
    lane = lax.broadcasted_iota(jnp.int32, (1, 128), 1)
    return [jnp.sum(jnp.where(lane == at, tile, 0.0), axis=1, keepdims=True) for at in range(count)]


def symmetric(six):
    a, b, c, d, e, f = six
    return [[a, b, c], [b, d, e], [c, e, f]]


def times(a, b):
    return [[sum(a[i][k] * b[k][j] for k in range(3)) for j in range(3)] for i in range(3)]


def turned(a):
    return [[a[j][i] for j in range(3)] for i in range(3)]


def minus(a, b):
    return [[a[i][j] - b[i][j] for j in range(3)] for i in range(3)]


def cholesky(h):
    zero = jnp.zeros_like(h[0][0])
    a = jnp.sqrt(h[0][0])
    b = h[1][0] / a
    c = h[2][0] / a
    d = jnp.sqrt(h[1][1] - b * b)
    e = (h[2][1] - c * b) / d
    f = jnp.sqrt(h[2][2] - c * c - e * e)
    return [[a, zero, zero], [b, d, zero], [c, e, f]]


def inverse(low):
    zero = jnp.zeros_like(low[0][0])
    a, d, f = 1.0 / low[0][0], 1.0 / low[1][1], 1.0 / low[2][2]
    b = -low[1][0] * a * d
    e = -low[2][1] * d * f
    c = -(low[2][0] * a + low[2][1] * b) * f
    return [[a, zero, zero], [b, d, zero], [c, e, f]]


def combine(matrix, vectors):
    return [sum(matrix[i][k] * vectors[k] for k in range(3)) for i in range(3)]


def place(row_index, forward_ref, sent_ref):
    for half in range(2):
        for k in range(3):
            sent_ref[2 * row_index + half, :, k * W : (k + 1) * W] = forward_ref[k : k + 1, half * W : (half + 1) * W]


def opening_kernel(mark_ref):
    mark_ref[...] = jnp.zeros_like(mark_ref)


def first_kernel(x_ref, d_ref, a_ref, mark_ref, sent_ref, flat_ref, diag_ref, high_ref, low_ref, x_rows, forward):
    row_index = lax.axis_index("row")
    x_rows[...] = jnp.zeros_like(x_rows)
    x_rows[0:3, :] = x_ref[...]
    for k in range(3):
        lanes = slice(k * W, (k + 1) * W)
        flat_ref[:, lanes] = x_ref[k : k + 1, :]
        diag_ref[:, lanes] = d_ref[...].reshape(1, W) - SHIFT
    x = flat_ref[...]
    for p in range(sent_ref.shape[0]):
        sent_ref[p] = x
    parts = three_parts(x_rows[...])
    for start in range(0, 2 * W, CHUNK):
        piece = slice(start, start + CHUNK)
        for at in range(start, start + CHUNK, STRIP):
            strip = slice(at, at + STRIP)
            block = a_ref[strip, :]
            high = block.astype(BF16)
            high_ref[strip, :] = high
            low_ref[strip, :] = (block - high.astype(F32)).astype(BF16)
        wide = over_rows(parts, high_ref[piece, :]) + over_rows(parts, low_ref[piece, :])
        forward[:, piece] = 0.5 * folded(wide)
    place(row_index, forward, sent_ref)


def forward_kernel(z_ref, x_ref, high_ref, low_ref, sent_ref, z_rows, forward):
    row_index = lax.axis_index("row")
    home = lax.axis_index("col") // 2 == row_index
    z = z_ref[...]
    z_rows[...] = jnp.zeros_like(z_rows)
    for k, row in enumerate(rows_of(z)):
        z_rows[k : k + 1, :] = row
    parts = three_parts(z_rows[...])
    six = rows_of(x_ref[...]) + rows_of(z)
    tile = packed(products_of([[row] for row in six]))
    head = jnp.where(home, z[:, 0:128], tile)
    for p in range(sent_ref.shape[0]):
        sent_ref[p, :, 0:128] = head
        sent_ref[p, :, 128:] = z[:, 128:]
    forward[...] = 0.5 * folded(over_rows(parts, high_ref[...]) + over_rows(parts, low_ref[...]))
    place(row_index, forward, sent_ref)


def first_backward_kernel(got_ref, own_ref, cross_ref, total_ref, high_ref, low_ref, sent_ref, v_rows):
    backward(got_ref, own_ref, cross_ref, total_ref, high_ref, low_ref, sent_ref, v_rows)


def second_backward_kernel(got_ref, own_ref, cross_ref, total_ref, tile_ref, high_ref, low_ref, sent_ref, v_rows):
    for p in range(sent_ref.shape[0]):
        sent_ref[p, :, FLAT:] = tile_ref[...]
    backward(got_ref, own_ref, cross_ref, total_ref, high_ref, low_ref, sent_ref, v_rows)


def backward(got_ref, own_ref, cross_ref, total_ref, high_ref, low_ref, sent_ref, v_rows):
    row_index = lax.axis_index("row")
    col_index = lax.axis_index("col")
    home = col_index // 2 == row_index
    v_rows[...] = jnp.zeros_like(v_rows)
    own = rows_of(own_ref[...])
    cross = rows_of(cross_ref[...]) if cross_ref.shape[0] == 1 else [cross_ref[k : k + 1, :] for k in range(3)]
    for half in range(2):
        sent_here = rows_of(got_ref[2 * row_index + half])
        for k in range(3):
            mine = jnp.where(col_index % 2 == half, own[k], cross[k])
            v_rows[k : k + 1, half * W : (half + 1) * W] = jnp.where(home, mine, sent_here[k])
    parts = three_parts(v_rows[...])
    total = rows_of(total_ref[...])
    wide = over_cols(parts, high_ref[...]) + over_cols(parts, low_ref[...])
    back = 0.5 * folded(wide)
    for k in range(3):
        part = back[k : k + 1] + total[k]
        for p in range(sent_ref.shape[0]):
            sent_ref[p, :, k * W : (k + 1) * W] = part


def sum_kernel(got_ref, total_ref):
    home = lax.axis_index("col") // 2 == lax.axis_index("row")
    total = got_ref[0]
    for p in range(1, got_ref.shape[0]):
        total = total + got_ref[p]
    total_ref[...] = jnp.where(home, total, 0.0)


def gram_kernel(got_ref, x_rows, total_ref, tile_ref):
    sum_kernel(got_ref, total_ref)
    row_index = lax.axis_index("row")
    tile = jnp.zeros((1, 128), F32)
    for p in range(got_ref.shape[0]):
        tile = tile + jnp.where(row_index == p // 2, 0.0, got_ref[p, :, 0:128])
    z = [rows_of(got_ref[2 * row_index + half]) for half in range(2)]
    rows = [[x_rows[k : k + 1, half * W : (half + 1) * W] for half in range(2)] for k in range(3)]
    rows += [[z[half][k] for half in range(2)] for k in range(3)]
    tile_ref[...] = tile + packed(products_of(rows))


def algebra(tile, coef_ref):
    flat = iter(unpacked(tile, 21))
    gram = {(i, j): next(flat) for i in range(6) for j in range(i, 6)}
    g00 = symmetric([gram[i, j] for i in range(3) for j in range(i, 3)])
    g01 = [[gram[i, j + 3] for j in range(3)] for i in range(3)]
    g11 = symmetric([gram[i + 3, j + 3] for i in range(3) for j in range(i, 3)])
    n0 = inverse(cholesky(g00))
    n0t = turned(n0)
    c0 = times(times(n0, turned(g01)), n0t)
    l1 = cholesky(minus(times(times(n0, g11), n0t), times(c0, turned(c0))))
    n1 = inverse(l1)
    at = 0
    for matrix in (n0, n1, c0, l1):
        for i in range(3):
            for j in range(3):
                coef_ref[at : at + 1, :] = jnp.broadcast_to(matrix[i][j], (1, 128))
                at += 1


def loaded(coef_ref, which, width):
    row = lambda at: coef_ref[at : at + 1, :]
    wide = lambda v: v if width == 128 else jnp.concatenate([v] * (width // 128), 1)
    return [[wide(row(9 * which + 3 * i + j)) for j in range(3)] for i in range(3)]


def residual_kernel(got_ref, z_ref, x_ref, d_ref, sent_ref, basis_ref, coef_ref):
    away = (lax.axis_index("col") // 2 + 1) % got_ref.shape[0]
    algebra(got_ref[away, :, FLAT:], coef_ref)
    total = got_ref[0, :, 0:FLAT]
    for p in range(1, got_ref.shape[0]):
        total = total + got_ref[p, :, 0:FLAT]
    z = z_ref[...]
    y = rows_of(total + d_ref[...] * z)
    n0, n1, c0, l1 = (loaded(coef_ref, i, W) for i in range(4))
    q0 = combine(n0, rows_of(x_ref[...]))
    u = combine(n0, rows_of(z))
    q1 = combine(n1, [a - b for a, b in zip(u, combine(c0, q0))])
    w = combine(n1, [a - b for a, b in zip(combine(n0, y), combine(c0, u))])
    known = [a + b for a, b in zip(combine(turned(l1), q0), combine(c0, q1))]
    w = [a - b for a, b in zip(w, known)]
    values = [inner(a, b) for a in w for b in q0 + q1]
    values += [inner(w[i], w[j]) for i in range(3) for j in range(i, 3)]
    tile = packed(values)
    for p in range(sent_ref.shape[0]):
        sent_ref[p] = tile
    for at, row in enumerate(q0 + q1 + w):
        basis_ref[at : at + 1, :] = row


def last_kernel(got_ref, basis_ref, coef_ref, out_ref, coeffs_ref):
    tile = got_ref[0]
    for p in range(1, got_ref.shape[0]):
        tile = tile + got_ref[p]
    values = unpacked(tile, 24)
    d0 = [values[6 * i : 6 * i + 3] for i in range(3)]
    d1 = [values[6 * i + 3 : 6 * i + 6] for i in range(3)]
    h2 = minus(minus(symmetric(values[18:]), times(d0, turned(d0))), times(d1, turned(d1)))
    l2 = cholesky(h2)
    n2 = inverse(l2)
    rows = [basis_ref[at : at + 1, :] for at in range(9)]
    q0, q1, w = rows[:3], rows[3:6], rows[6:]
    known = [a + b for a, b in zip(combine(d0, q0), combine(d1, q1))]
    q2 = combine(n2, [a - b for a, b in zip(w, known)])
    root = float(M) ** 0.5
    for k in range(3):
        out_ref[k, 0:1, :] = q1[k] * root
        out_ref[k, 1:2, :] = q2[k] * root
    c0, l1 = ([[v[:, 0:1] for v in line] for line in loaded(coef_ref, i, 128)] for i in (2, 3))
    down = lax.broadcasted_iota(jnp.int32, (3, 3), 0)
    across = lax.broadcasted_iota(jnp.int32, (3, 3), 1)

    def square(matrix, shift):
        tile = jnp.where(down == across, shift, 0.0)
        for i in range(3):
            for j in range(3):
                tile = jnp.where((down == i) & (across == j), tile + matrix[i][j], tile)
        return tile

    second = [[c0[i][j] + d1[i][j] for j in range(3)] for i in range(3)]
    blocks = [[square(c0, SHIFT), square(l1, 0.0)], [square(second, SHIFT), square(l2, 0.0)]]
    for j in range(2):
        for i in range(3):
            for which in range(2):
                coeffs_ref[j, i, which : which + 1, :] = blocks[j][which][i : i + 1, :]


def collect_kernel(got_ref, d_ref, x_ref, z_ref):
    total = got_ref[0]
    for p in range(1, got_ref.shape[0]):
        total = total + got_ref[p]
    z_ref[...] = total + d_ref[...] * x_ref[...]


def call(kernel, out, inputs, scratch=(), specs=None, out_specs=None, flops=2_000_000):
    return pl.pallas_call(
        kernel,
        out_shape=out,
        in_specs=specs or [VMEM] * len(inputs),
        out_specs=out_specs or jax.tree.map(lambda _: VMEM, out),
        scratch_shapes=list(scratch),
        cost_estimate=pl.CostEstimate(flops=flops, bytes_accessed=100_000, transcendentals=0),
        compiler_params=pltpu.CompilerParams(vmem_limit_bytes=24 << 20),
    )(*inputs)


def shards(couplings, diag_terms, start_block):
    cols = lax.axis_size("col")
    rows = lax.axis_size("row")
    swap = [(i, i ^ 1) for i in range(cols)]
    whole = (2 * W, W)
    tall = pltpu.VMEM((8, 2 * W), F32)
    short = pltpu.VMEM((8, W), F32)
    flat = in_vmem((1, FLAT))

    def exchanged(block, axis):
        return lax.all_to_all(block, axis, 0, 0, tiled=True)

    def spread(sent, block):
        cross = lax.ppermute(block, "col", swap)
        return exchanged(sent, "col"), cross

    mark = call(opening_kernel, in_vmem((8, 128)), (), flops=5_000_000_000)
    held, mark = lax.optimization_barrier((start_block, mark))
    cross = lax.ppermute(held, "col", swap)
    sent, x, d, high, low = call(
        first_kernel,
        (in_vmem((cols, 1, FLAT)), flat, flat, in_vmem(whole, BF16), in_vmem(whole, BF16)),
        (start_block, diag_terms, couplings, mark),
        [short, tall],
    )
    got = exchanged(sent, "col")
    total = call(sum_kernel, flat, (got,))
    many = in_vmem((8, 2 * W))
    sent, x_rows = call(
        first_backward_kernel, (in_vmem((rows, 1, FLAT)), many), (got, x, cross, total, high, low)
    )
    got = exchanged(sent, "row")
    z = call(collect_kernel, flat, (got, d, x))
    sent = call(forward_kernel, in_vmem((cols, 1, FLAT)), (z, x, high, low), [short, tall])
    got, cross = spread(sent, z)
    total, tile = call(gram_kernel, (flat, in_vmem((1, 128))), (got, x_rows))
    sent = call(
        second_backward_kernel,
        in_vmem((rows, 1, FLAT + 128)),
        (got, z, cross, total, tile, high, low),
        [tall],
    )
    got = exchanged(sent, "row")
    sent, basis, coef = call(
        residual_kernel,
        (in_vmem((cols, 1, 128)), in_vmem((16, W)), in_vmem((40, 128))),
        (got, z, x, d),
    )
    got = exchanged(sent, "col")
    f32 = lambda *shape: jax.ShapeDtypeStruct(shape, F32)
    blocks, coeffs = call(last_kernel, (f32(3, 2, W), f32(2, 3, 2, 3)), (got, basis, coef))
    return jnp.swapaxes(blocks, 0, 1), jnp.swapaxes(coeffs, 1, 2)


def solution(mesh):
    placed = (P("row", "col"), P("col"), P(None, "col"))
    return jax.shard_map(
        shards, mesh=mesh, in_specs=placed, out_specs=(P(None, None, "col"), P()), check_vma=False
    )
```

```python
import jax
import jax.numpy as jnp
from jax import lax
from jax.experimental import pallas as pl
from jax.experimental.pallas import tpu as pltpu
from jax.sharding import PartitionSpec as P


M = 24576
SHIFT = 2.5
W = 768
FLAT = 3 * W
CHUNK = 512
STRIP = 16
F32 = jnp.float32
BF16 = jnp.bfloat16
VMEM = pl.BlockSpec(memory_space=pltpu.VMEM)
HBM = pl.BlockSpec(memory_space=pltpu.HBM)


def in_vmem(shape, dtype=F32):
    return pltpu.VMEM(shape, dtype)


def three_parts(x):
    first = x.astype(BF16).astype(F32)
    rest = x - first
    second = rest.astype(BF16).astype(F32)
    return jnp.concatenate([first, second, rest - second], 0).astype(BF16)


def folded(wide):
    return wide[0:8] + wide[8:16] + wide[16:24]


def over_rows(parts, matrix):
    return lax.dot_general(parts, matrix, (((1,), (1,)), ((), ())), preferred_element_type=F32)


def over_cols(parts, matrix):
    return lax.dot_general(parts, matrix, (((1,), (0,)), ((), ())), preferred_element_type=F32)


def rows_of(flat):
    return [flat[:, k * W : (k + 1) * W] for k in range(3)]


def inner(a, b):
    return jnp.sum(a * b, axis=1, keepdims=True)


def packed(values):
    lane = lax.broadcasted_iota(jnp.int32, (1, 128), 1)
    tile = jnp.zeros((1, 128), F32)
    for at, value in enumerate(values):
        tile = jnp.where(lane == at, value, tile)
    return tile


def products_of(rows):
    return [sum(inner(a, b) for a, b in zip(rows[i], rows[j])) for i in range(6) for j in range(i, 6)]


def unpacked(tile, count):
    lane = lax.broadcasted_iota(jnp.int32, (1, 128), 1)
    return [jnp.sum(jnp.where(lane == at, tile, 0.0), axis=1, keepdims=True) for at in range(count)]


def symmetric(six):
    a, b, c, d, e, f = six
    return [[a, b, c], [b, d, e], [c, e, f]]


def times(a, b):
    return [[sum(a[i][k] * b[k][j] for k in range(3)) for j in range(3)] for i in range(3)]


def turned(a):
    return [[a[j][i] for j in range(3)] for i in range(3)]


def minus(a, b):
    return [[a[i][j] - b[i][j] for j in range(3)] for i in range(3)]


def cholesky(h):
    zero = jnp.zeros_like(h[0][0])
    a = jnp.sqrt(h[0][0])
    b = h[1][0] / a
    c = h[2][0] / a
    d = jnp.sqrt(h[1][1] - b * b)
    e = (h[2][1] - c * b) / d
    f = jnp.sqrt(h[2][2] - c * c - e * e)
    return [[a, zero, zero], [b, d, zero], [c, e, f]]


def inverse(low):
    zero = jnp.zeros_like(low[0][0])
    a, d, f = 1.0 / low[0][0], 1.0 / low[1][1], 1.0 / low[2][2]
    b = -low[1][0] * a * d
    e = -low[2][1] * d * f
    c = -(low[2][0] * a + low[2][1] * b) * f
    return [[a, zero, zero], [b, d, zero], [c, e, f]]


def combine(matrix, vectors):
    return [sum(matrix[i][k] * vectors[k] for k in range(3)) for i in range(3)]


def place(row_index, forward_ref, sent_ref):
    for half in range(2):
        for k in range(3):
            sent_ref[2 * row_index + half, :, k * W : (k + 1) * W] = forward_ref[k : k + 1, half * W : (half + 1) * W]


def opening_kernel(mark_ref):
    mark_ref[...] = jnp.zeros_like(mark_ref)


def first_kernel(x_ref, d_ref, a_ref, mark_ref, sent_ref, flat_ref, diag_ref, high_ref, low_ref, x_rows, forward):
    row_index = lax.axis_index("row")
    x_rows[...] = jnp.zeros_like(x_rows)
    x_rows[0:3, :] = x_ref[...]
    for k in range(3):
        lanes = slice(k * W, (k + 1) * W)
        flat_ref[:, lanes] = x_ref[k : k + 1, :]
        diag_ref[:, lanes] = d_ref[...].reshape(1, W) - SHIFT
    x = flat_ref[...]
    for p in range(sent_ref.shape[0]):
        sent_ref[p] = x
    parts = three_parts(x_rows[...])
    for start in range(0, 2 * W, CHUNK):
        piece = slice(start, start + CHUNK)
        for at in range(start, start + CHUNK, STRIP):
            strip = slice(at, at + STRIP)
            block = a_ref[strip, :]
            high = block.astype(BF16)
            high_ref[strip, :] = high
            low_ref[strip, :] = (block - high.astype(F32)).astype(BF16)
        wide = over_rows(parts, high_ref[piece, :]) + over_rows(parts, low_ref[piece, :])
        forward[:, piece] = 0.5 * folded(wide)
    place(row_index, forward, sent_ref)


def forward_kernel(z_ref, x_ref, high_ref, low_ref, sent_ref, z_rows, forward):
    row_index = lax.axis_index("row")
    home = lax.axis_index("col") // 2 == row_index
    z = z_ref[...]
    z_rows[...] = jnp.zeros_like(z_rows)
    for k, row in enumerate(rows_of(z)):
        z_rows[k : k + 1, :] = row
    parts = three_parts(z_rows[...])
    six = rows_of(x_ref[...]) + rows_of(z)
    tile = packed(products_of([[row] for row in six]))
    head = jnp.where(home, z[:, 0:128], tile)
    for p in range(sent_ref.shape[0]):
        sent_ref[p, :, 0:128] = head
        sent_ref[p, :, 128:] = z[:, 128:]
    forward[...] = 0.5 * folded(over_rows(parts, high_ref[...]) + over_rows(parts, low_ref[...]))
    place(row_index, forward, sent_ref)


def first_backward_kernel(got_ref, own_ref, cross_ref, total_ref, high_ref, low_ref, sent_ref, v_rows):
    backward(got_ref, own_ref, cross_ref, total_ref, high_ref, low_ref, sent_ref, v_rows)


def second_backward_kernel(
    got_ref, own_ref, cross_ref, x_rows, high_ref, low_hbm, sent_ref, low, v_rows, total_ref, tile_ref, wide_ref, sems
):
    pieces = [slice(start, start + CHUNK) for start in range(0, 2 * W, CHUNK)]
    copies = [pltpu.make_async_copy(low_hbm.at[piece], low.at[piece], sems.at[i]) for i, piece in enumerate(pieces)]
    for copy in copies:
        copy.start()
    assemble(got_ref, own_ref, cross_ref, v_rows)
    parts = three_parts(v_rows[...])
    wide_ref[...] = over_cols(parts, high_ref[...])
    gram_kernel(got_ref, x_rows, total_ref, tile_ref)
    for p in range(sent_ref.shape[0]):
        sent_ref[p, :, FLAT:] = tile_ref[...]
    total = rows_of(total_ref[...])
    wide = wide_ref[...]
    for copy, piece in zip(copies, pieces):
        copy.wait()
        wide = wide + over_cols(parts[:, piece], low[piece, :])
    deliver(0.5 * folded(wide), total, sent_ref)


def backward(got_ref, own_ref, cross_ref, total_ref, high_ref, low_ref, sent_ref, v_rows):
    assemble(got_ref, own_ref, cross_ref, v_rows)
    parts = three_parts(v_rows[...])
    wide = over_cols(parts, high_ref[...]) + over_cols(parts, low_ref[...])
    deliver(0.5 * folded(wide), rows_of(total_ref[...]), sent_ref)


def deliver(back, total, sent_ref):
    for k in range(3):
        part = back[k : k + 1] + total[k]
        for p in range(sent_ref.shape[0]):
            sent_ref[p, :, k * W : (k + 1) * W] = part


def assemble(got_ref, own_ref, cross_ref, v_rows):
    row_index = lax.axis_index("row")
    col_index = lax.axis_index("col")
    home = col_index // 2 == row_index
    v_rows[...] = jnp.zeros_like(v_rows)
    own = rows_of(own_ref[...])
    cross = rows_of(cross_ref[...]) if cross_ref.shape[0] == 1 else [cross_ref[k : k + 1, :] for k in range(3)]
    for half in range(2):
        sent_here = rows_of(got_ref[2 * row_index + half])
        for k in range(3):
            mine = jnp.where(col_index % 2 == half, own[k], cross[k])
            v_rows[k : k + 1, half * W : (half + 1) * W] = jnp.where(home, mine, sent_here[k])


def sum_kernel(got_ref, total_ref):
    home = lax.axis_index("col") // 2 == lax.axis_index("row")
    total = got_ref[0]
    for p in range(1, got_ref.shape[0]):
        total = total + got_ref[p]
    total_ref[...] = jnp.where(home, total, 0.0)


def gram_kernel(got_ref, x_rows, total_ref, tile_ref):
    sum_kernel(got_ref, total_ref)
    row_index = lax.axis_index("row")
    tile = jnp.zeros((1, 128), F32)
    for p in range(got_ref.shape[0]):
        tile = tile + jnp.where(row_index == p // 2, 0.0, got_ref[p, :, 0:128])
    z = [rows_of(got_ref[2 * row_index + half]) for half in range(2)]
    rows = [[x_rows[k : k + 1, half * W : (half + 1) * W] for half in range(2)] for k in range(3)]
    rows += [[z[half][k] for half in range(2)] for k in range(3)]
    tile_ref[...] = tile + packed(products_of(rows))


def algebra(tile, coef_ref):
    flat = iter(unpacked(tile, 21))
    gram = {(i, j): next(flat) for i in range(6) for j in range(i, 6)}
    g00 = symmetric([gram[i, j] for i in range(3) for j in range(i, 3)])
    g01 = [[gram[i, j + 3] for j in range(3)] for i in range(3)]
    g11 = symmetric([gram[i + 3, j + 3] for i in range(3) for j in range(i, 3)])
    n0 = inverse(cholesky(g00))
    n0t = turned(n0)
    c0 = times(times(n0, turned(g01)), n0t)
    l1 = cholesky(minus(times(times(n0, g11), n0t), times(c0, turned(c0))))
    n1 = inverse(l1)
    at = 0
    for matrix in (n0, n1, c0, l1):
        for i in range(3):
            for j in range(3):
                coef_ref[at : at + 1, :] = jnp.broadcast_to(matrix[i][j], (1, 128))
                at += 1


def loaded(coef_ref, which, width):
    row = lambda at: coef_ref[at : at + 1, :]
    wide = lambda v: v if width == 128 else jnp.concatenate([v] * (width // 128), 1)
    return [[wide(row(9 * which + 3 * i + j)) for j in range(3)] for i in range(3)]


def residual_kernel(got_ref, z_ref, x_ref, d_ref, sent_ref, basis_ref, coef_ref):
    away = (lax.axis_index("col") // 2 + 1) % got_ref.shape[0]
    algebra(got_ref[away, :, FLAT:], coef_ref)
    total = got_ref[0, :, 0:FLAT]
    for p in range(1, got_ref.shape[0]):
        total = total + got_ref[p, :, 0:FLAT]
    z = z_ref[...]
    y = rows_of(total + d_ref[...] * z)
    n0, n1, c0, l1 = (loaded(coef_ref, i, W) for i in range(4))
    q0 = combine(n0, rows_of(x_ref[...]))
    u = combine(n0, rows_of(z))
    q1 = combine(n1, [a - b for a, b in zip(u, combine(c0, q0))])
    w = combine(n1, [a - b for a, b in zip(combine(n0, y), combine(c0, u))])
    known = [a + b for a, b in zip(combine(turned(l1), q0), combine(c0, q1))]
    w = [a - b for a, b in zip(w, known)]
    values = [inner(a, b) for a in w for b in q0 + q1]
    values += [inner(w[i], w[j]) for i in range(3) for j in range(i, 3)]
    tile = packed(values)
    for p in range(sent_ref.shape[0]):
        sent_ref[p] = tile
    for at, row in enumerate(q0 + q1 + w):
        basis_ref[at : at + 1, :] = row


def last_kernel(got_ref, basis_ref, coef_ref, out_ref, coeffs_ref):
    tile = got_ref[0]
    for p in range(1, got_ref.shape[0]):
        tile = tile + got_ref[p]
    values = unpacked(tile, 24)
    d0 = [values[6 * i : 6 * i + 3] for i in range(3)]
    d1 = [values[6 * i + 3 : 6 * i + 6] for i in range(3)]
    h2 = minus(minus(symmetric(values[18:]), times(d0, turned(d0))), times(d1, turned(d1)))
    l2 = cholesky(h2)
    n2 = inverse(l2)
    rows = [basis_ref[at : at + 1, :] for at in range(9)]
    q0, q1, w = rows[:3], rows[3:6], rows[6:]
    known = [a + b for a, b in zip(combine(d0, q0), combine(d1, q1))]
    q2 = combine(n2, [a - b for a, b in zip(w, known)])
    root = float(M) ** 0.5
    for k in range(3):
        out_ref[k, 0:1, :] = q1[k] * root
        out_ref[k, 1:2, :] = q2[k] * root
    c0, l1 = ([[v[:, 0:1] for v in line] for line in loaded(coef_ref, i, 128)] for i in (2, 3))
    down = lax.broadcasted_iota(jnp.int32, (3, 3), 0)
    across = lax.broadcasted_iota(jnp.int32, (3, 3), 1)

    def square(matrix, shift):
        tile = jnp.where(down == across, shift, 0.0)
        for i in range(3):
            for j in range(3):
                tile = jnp.where((down == i) & (across == j), tile + matrix[i][j], tile)
        return tile

    second = [[c0[i][j] + d1[i][j] for j in range(3)] for i in range(3)]
    blocks = [[square(c0, SHIFT), square(l1, 0.0)], [square(second, SHIFT), square(l2, 0.0)]]
    for j in range(2):
        for i in range(3):
            for which in range(2):
                coeffs_ref[j, i, which : which + 1, :] = blocks[j][which][i : i + 1, :]


def collect_kernel(got_ref, d_ref, x_ref, z_ref):
    total = got_ref[0]
    for p in range(1, got_ref.shape[0]):
        total = total + got_ref[p]
    z_ref[...] = total + d_ref[...] * x_ref[...]


def call(kernel, out, inputs, scratch=(), specs=None, out_specs=None, flops=2_000_000):
    return pl.pallas_call(
        kernel,
        out_shape=out,
        in_specs=specs or [VMEM] * len(inputs),
        out_specs=out_specs or jax.tree.map(lambda _: VMEM, out),
        scratch_shapes=list(scratch),
        cost_estimate=pl.CostEstimate(flops=flops, bytes_accessed=100_000, transcendentals=0),
        compiler_params=pltpu.CompilerParams(vmem_limit_bytes=24 << 20),
    )(*inputs)


def shards(couplings, diag_terms, start_block):
    cols = lax.axis_size("col")
    rows = lax.axis_size("row")
    swap = [(i, i ^ 1) for i in range(cols)]
    whole = (2 * W, W)
    tall = pltpu.VMEM((8, 2 * W), F32)
    short = pltpu.VMEM((8, W), F32)
    flat = in_vmem((1, FLAT))

    def exchanged(block, axis):
        return lax.all_to_all(block, axis, 0, 0, tiled=True)

    mark = call(opening_kernel, in_vmem((8, 128)), (), flops=5_000_000_000)
    held, mark = lax.optimization_barrier((start_block, mark))
    cross = lax.ppermute(held, "col", swap)
    sent, x, d, high, low = call(
        first_kernel,
        (in_vmem((cols, 1, FLAT)), flat, flat, in_vmem(whole, BF16), in_vmem(whole, BF16)),
        (start_block, diag_terms, couplings, mark),
        [short, tall],
    )
    got = exchanged(sent, "col")
    total = call(sum_kernel, flat, (got,))
    many = in_vmem((8, 2 * W))
    sent, x_rows = call(
        first_backward_kernel, (in_vmem((rows, 1, FLAT)), many), (got, x, cross, total, high, low)
    )
    got = exchanged(sent, "row")
    z = call(collect_kernel, flat, (got, d, x))
    slots = jax.ShapeDtypeStruct((cols, 1, FLAT), F32)
    sent = call(forward_kernel, slots, (z, x, high, low), [short, tall])
    cross = lax.ppermute(z, "col", swap)
    got = exchanged(sent, "col")
    sent = call(
        second_backward_kernel,
        in_vmem((rows, 1, FLAT + 128)),
        (got, z, cross, x_rows, high, pltpu.with_memory_space_constraint(low, pltpu.HBM)),
        [
            pltpu.VMEM(whole, BF16),
            tall,
            pltpu.VMEM((1, FLAT), F32),
            pltpu.VMEM((1, 128), F32),
            pltpu.VMEM((24, W), F32),
            pltpu.SemaphoreType.DMA((2 * W // CHUNK,)),
        ],
        [VMEM] * 5 + [HBM],
    )
    got = exchanged(sent, "row")
    sent, basis, coef = call(
        residual_kernel,
        (in_vmem((cols, 1, 128)), in_vmem((16, W)), in_vmem((40, 128))),
        (got, z, x, d),
    )
    got = exchanged(sent, "col")
    f32 = lambda *shape: jax.ShapeDtypeStruct(shape, F32)
    blocks, coeffs = call(last_kernel, (f32(3, 2, W), f32(2, 3, 2, 3)), (got, basis, coef))
    return jnp.swapaxes(blocks, 0, 1), jnp.swapaxes(coeffs, 1, 2)


def solution(mesh):
    placed = (P("row", "col"), P("col"), P(None, "col"))
    return jax.shard_map(
        shards, mesh=mesh, in_specs=placed, out_specs=(P(None, None, "col"), P()), check_vma=False
    )
```

```python
import jax
import jax.numpy as jnp
from jax import lax
from jax.experimental import pallas as pl
from jax.experimental.pallas import tpu as pltpu
from jax.sharding import PartitionSpec as P


M = 24576
SHIFT = 2.5
W = 768
FLAT = 3 * W
CHUNK = 512
STRIP = 16
F32 = jnp.float32
BF16 = jnp.bfloat16
VMEM = pl.BlockSpec(memory_space=pltpu.VMEM)
HBM = pl.BlockSpec(memory_space=pltpu.HBM)


def in_vmem(shape, dtype=F32):
    return pltpu.VMEM(shape, dtype)


def three_parts(x):
    first = x.astype(BF16).astype(F32)
    rest = x - first
    second = rest.astype(BF16).astype(F32)
    return jnp.concatenate([first, second, rest - second], 0).astype(BF16)


def folded(wide):
    return wide[0:8] + wide[8:16] + wide[16:24]


def over_rows(parts, matrix):
    return lax.dot_general(parts, matrix, (((1,), (1,)), ((), ())), preferred_element_type=F32)


def over_cols(parts, matrix):
    return lax.dot_general(parts, matrix, (((1,), (0,)), ((), ())), preferred_element_type=F32)


def rows_of(flat):
    return [flat[:, k * W : (k + 1) * W] for k in range(3)]


def inner(a, b):
    return jnp.sum(a * b, axis=1, keepdims=True)


def packed(values):
    lane = lax.broadcasted_iota(jnp.int32, (1, 128), 1)
    tile = jnp.zeros((1, 128), F32)
    for at, value in enumerate(values):
        tile = jnp.where(lane == at, value, tile)
    return tile


def products_of(rows):
    return [sum(inner(a, b) for a, b in zip(rows[i], rows[j])) for i in range(6) for j in range(i, 6)]


def unpacked(tile, count):
    lane = lax.broadcasted_iota(jnp.int32, (1, 128), 1)
    return [jnp.sum(jnp.where(lane == at, tile, 0.0), axis=1, keepdims=True) for at in range(count)]


def symmetric(six):
    a, b, c, d, e, f = six
    return [[a, b, c], [b, d, e], [c, e, f]]


def times(a, b):
    return [[sum(a[i][k] * b[k][j] for k in range(3)) for j in range(3)] for i in range(3)]


def turned(a):
    return [[a[j][i] for j in range(3)] for i in range(3)]


def minus(a, b):
    return [[a[i][j] - b[i][j] for j in range(3)] for i in range(3)]


def cholesky(h):
    zero = jnp.zeros_like(h[0][0])
    a = jnp.sqrt(h[0][0])
    b = h[1][0] / a
    c = h[2][0] / a
    d = jnp.sqrt(h[1][1] - b * b)
    e = (h[2][1] - c * b) / d
    f = jnp.sqrt(h[2][2] - c * c - e * e)
    return [[a, zero, zero], [b, d, zero], [c, e, f]]


def inverse(low):
    zero = jnp.zeros_like(low[0][0])
    a, d, f = 1.0 / low[0][0], 1.0 / low[1][1], 1.0 / low[2][2]
    b = -low[1][0] * a * d
    e = -low[2][1] * d * f
    c = -(low[2][0] * a + low[2][1] * b) * f
    return [[a, zero, zero], [b, d, zero], [c, e, f]]


def combine(matrix, vectors):
    return [sum(matrix[i][k] * vectors[k] for k in range(3)) for i in range(3)]


def place(row_index, forward_ref, sent_ref):
    for half in range(2):
        for k in range(3):
            sent_ref[2 * row_index + half, :, k * W : (k + 1) * W] = forward_ref[k : k + 1, half * W : (half + 1) * W]


def opening_kernel(mark_ref):
    mark_ref[...] = jnp.zeros_like(mark_ref)


def first_kernel(x_ref, d_ref, a_ref, mark_ref, sent_ref, flat_ref, diag_ref, high_ref, near_ref, far_ref, x_rows, forward):
    row_index = lax.axis_index("row")
    x_rows[...] = jnp.zeros_like(x_rows)
    x_rows[0:3, :] = x_ref[...]
    for k in range(3):
        lanes = slice(k * W, (k + 1) * W)
        flat_ref[:, lanes] = x_ref[k : k + 1, :]
        diag_ref[:, lanes] = d_ref[...].reshape(1, W) - SHIFT
    x = flat_ref[...]
    for p in range(sent_ref.shape[0]):
        sent_ref[p] = x
    parts = three_parts(x_rows[...])
    for start in range(0, 2 * W, CHUNK):
        piece = slice(start, start + CHUNK)
        low_ref, base = (near_ref, 0) if start == 0 else (far_ref, CHUNK)
        for at in range(start, start + CHUNK, STRIP):
            block = a_ref[at : at + STRIP, :]
            high = block.astype(BF16)
            high_ref[at : at + STRIP, :] = high
            low_ref[at - base : at - base + STRIP, :] = (block - high.astype(F32)).astype(BF16)
        low = low_ref[start - base : start - base + CHUNK, :]
        wide = over_rows(parts, high_ref[piece, :]) + over_rows(parts, low)
        forward[:, piece] = 0.5 * folded(wide)
    place(row_index, forward, sent_ref)


def forward_kernel(z_ref, x_ref, high_ref, near_ref, far_ref, sent_hbm, sent_ref, pair_ref, z_rows, forward, sems):
    row_index = lax.axis_index("row")
    home = lax.axis_index("col") // 2 == row_index
    z = z_ref[...]
    z_rows[...] = jnp.zeros_like(z_rows)
    for k, row in enumerate(rows_of(z)):
        z_rows[k : k + 1, :] = row
    parts = three_parts(z_rows[...])
    six = rows_of(x_ref[...]) + rows_of(z)
    tile = packed(products_of([[row] for row in six]))
    head = jnp.where(home, z[:, 0:128], tile)
    for p in range(sent_ref.shape[0]):
        sent_ref[p, :, 0:128] = head
        sent_ref[p, :, 128:] = z[:, 128:]
    filled = pltpu.make_async_copy(sent_ref, sent_hbm, sems.at[0])
    filled.start()
    for piece, low_ref in ((slice(0, CHUNK), near_ref), (slice(CHUNK, 2 * W), far_ref)):
        wide = over_rows(parts, high_ref[piece, :]) + over_rows(parts, low_ref[...])
        forward[:, piece] = 0.5 * folded(wide)
    place(0, forward, pair_ref)
    aimed = pltpu.make_async_copy(pair_ref, sent_hbm.at[pl.ds(2 * row_index, 2)], sems.at[1])
    filled.wait()
    aimed.start()
    aimed.wait()


def first_backward_kernel(got_ref, own_ref, cross_ref, total_ref, high_ref, near_ref, far_ref, sent_ref, v_rows):
    assemble(got_ref, own_ref, cross_ref, v_rows)
    parts = three_parts(v_rows[...])
    wide = over_cols(parts, high_ref[...]) + over_cols(parts[:, :CHUNK], near_ref[...])
    wide = wide + over_cols(parts[:, CHUNK:], far_ref[...])
    deliver(0.5 * folded(wide), rows_of(total_ref[...]), sent_ref)


def second_backward_kernel(
    got_ref, own_ref, cross_ref, x_rows, high_ref, near_ref, far_hbm, sent_ref, far, v_rows, total_ref, tile_ref, wide_ref, sems
):
    pieces = [slice(start, start + CHUNK) for start in range(0, far.shape[0], CHUNK)]
    copies = [pltpu.make_async_copy(far_hbm.at[piece], far.at[piece], sems.at[i]) for i, piece in enumerate(pieces)]
    for copy in copies:
        copy.start()
    assemble(got_ref, own_ref, cross_ref, v_rows)
    parts = three_parts(v_rows[...])
    wide_ref[...] = over_cols(parts, high_ref[...]) + over_cols(parts[:, :CHUNK], near_ref[...])
    gram_kernel(got_ref, x_rows, total_ref, tile_ref)
    for p in range(sent_ref.shape[0]):
        sent_ref[p, :, FLAT:] = tile_ref[...]
    total = rows_of(total_ref[...])
    wide = wide_ref[...]
    for copy, piece in zip(copies, pieces):
        copy.wait()
        wide = wide + over_cols(parts[:, CHUNK + piece.start : CHUNK + piece.stop], far[piece, :])
    deliver(0.5 * folded(wide), total, sent_ref)


def deliver(back, total, sent_ref):
    for k in range(3):
        part = back[k : k + 1] + total[k]
        for p in range(sent_ref.shape[0]):
            sent_ref[p, :, k * W : (k + 1) * W] = part


def assemble(got_ref, own_ref, cross_ref, v_rows):
    row_index = lax.axis_index("row")
    col_index = lax.axis_index("col")
    home = col_index // 2 == row_index
    v_rows[...] = jnp.zeros_like(v_rows)
    own = rows_of(own_ref[...])
    cross = rows_of(cross_ref[...]) if cross_ref.shape[0] == 1 else [cross_ref[k : k + 1, :] for k in range(3)]
    for half in range(2):
        sent_here = rows_of(got_ref[2 * row_index + half])
        for k in range(3):
            mine = jnp.where(col_index % 2 == half, own[k], cross[k])
            v_rows[k : k + 1, half * W : (half + 1) * W] = jnp.where(home, mine, sent_here[k])


def sum_kernel(got_ref, total_ref):
    home = lax.axis_index("col") // 2 == lax.axis_index("row")
    total = got_ref[0]
    for p in range(1, got_ref.shape[0]):
        total = total + got_ref[p]
    total_ref[...] = jnp.where(home, total, 0.0)


def gram_kernel(got_ref, x_rows, total_ref, tile_ref):
    sum_kernel(got_ref, total_ref)
    row_index = lax.axis_index("row")
    tile = jnp.zeros((1, 128), F32)
    for p in range(got_ref.shape[0]):
        tile = tile + jnp.where(row_index == p // 2, 0.0, got_ref[p, :, 0:128])
    z = [rows_of(got_ref[2 * row_index + half]) for half in range(2)]
    rows = [[x_rows[k : k + 1, half * W : (half + 1) * W] for half in range(2)] for k in range(3)]
    rows += [[z[half][k] for half in range(2)] for k in range(3)]
    tile_ref[...] = tile + packed(products_of(rows))


def algebra(tile, coef_ref):
    flat = iter(unpacked(tile, 21))
    gram = {(i, j): next(flat) for i in range(6) for j in range(i, 6)}
    g00 = symmetric([gram[i, j] for i in range(3) for j in range(i, 3)])
    g01 = [[gram[i, j + 3] for j in range(3)] for i in range(3)]
    g11 = symmetric([gram[i + 3, j + 3] for i in range(3) for j in range(i, 3)])
    n0 = inverse(cholesky(g00))
    n0t = turned(n0)
    c0 = times(times(n0, turned(g01)), n0t)
    l1 = cholesky(minus(times(times(n0, g11), n0t), times(c0, turned(c0))))
    n1 = inverse(l1)
    at = 0
    for matrix in (n0, n1, c0, l1):
        for i in range(3):
            for j in range(3):
                coef_ref[at : at + 1, :] = jnp.broadcast_to(matrix[i][j], (1, 128))
                at += 1


def loaded(coef_ref, which, width):
    row = lambda at: coef_ref[at : at + 1, :]
    wide = lambda v: v if width == 128 else jnp.concatenate([v] * (width // 128), 1)
    return [[wide(row(9 * which + 3 * i + j)) for j in range(3)] for i in range(3)]


def residual_kernel(got_ref, z_ref, x_ref, d_ref, sent_ref, basis_ref, coef_ref):
    away = (lax.axis_index("col") // 2 + 1) % got_ref.shape[0]
    algebra(got_ref[away, :, FLAT:], coef_ref)
    total = got_ref[0, :, 0:FLAT]
    for p in range(1, got_ref.shape[0]):
        total = total + got_ref[p, :, 0:FLAT]
    z = z_ref[...]
    y = rows_of(total + d_ref[...] * z)
    n0, n1, c0, l1 = (loaded(coef_ref, i, W) for i in range(4))
    q0 = combine(n0, rows_of(x_ref[...]))
    u = combine(n0, rows_of(z))
    q1 = combine(n1, [a - b for a, b in zip(u, combine(c0, q0))])
    w = combine(n1, [a - b for a, b in zip(combine(n0, y), combine(c0, u))])
    known = [a + b for a, b in zip(combine(turned(l1), q0), combine(c0, q1))]
    w = [a - b for a, b in zip(w, known)]
    values = [inner(a, b) for a in w for b in q0 + q1]
    values += [inner(w[i], w[j]) for i in range(3) for j in range(i, 3)]
    tile = packed(values)
    for p in range(sent_ref.shape[0]):
        sent_ref[p] = tile
    for at, row in enumerate(q0 + q1 + w):
        basis_ref[at : at + 1, :] = row


def last_kernel(got_ref, basis_ref, coef_ref, out_ref, coeffs_ref):
    tile = got_ref[0]
    for p in range(1, got_ref.shape[0]):
        tile = tile + got_ref[p]
    values = unpacked(tile, 24)
    d0 = [values[6 * i : 6 * i + 3] for i in range(3)]
    d1 = [values[6 * i + 3 : 6 * i + 6] for i in range(3)]
    h2 = minus(minus(symmetric(values[18:]), times(d0, turned(d0))), times(d1, turned(d1)))
    l2 = cholesky(h2)
    n2 = inverse(l2)
    rows = [basis_ref[at : at + 1, :] for at in range(9)]
    q0, q1, w = rows[:3], rows[3:6], rows[6:]
    known = [a + b for a, b in zip(combine(d0, q0), combine(d1, q1))]
    q2 = combine(n2, [a - b for a, b in zip(w, known)])
    root = float(M) ** 0.5
    for k in range(3):
        out_ref[k, 0:1, :] = q1[k] * root
        out_ref[k, 1:2, :] = q2[k] * root
    c0, l1 = ([[v[:, 0:1] for v in line] for line in loaded(coef_ref, i, 128)] for i in (2, 3))
    down = lax.broadcasted_iota(jnp.int32, (3, 3), 0)
    across = lax.broadcasted_iota(jnp.int32, (3, 3), 1)

    def square(matrix, shift):
        tile = jnp.where(down == across, shift, 0.0)
        for i in range(3):
            for j in range(3):
                tile = jnp.where((down == i) & (across == j), tile + matrix[i][j], tile)
        return tile

    second = [[c0[i][j] + d1[i][j] for j in range(3)] for i in range(3)]
    blocks = [[square(c0, SHIFT), square(l1, 0.0)], [square(second, SHIFT), square(l2, 0.0)]]
    for j in range(2):
        for i in range(3):
            for which in range(2):
                coeffs_ref[j, i, which : which + 1, :] = blocks[j][which][i : i + 1, :]


def collect_kernel(got_ref, d_ref, x_ref, z_ref):
    total = got_ref[0]
    for p in range(1, got_ref.shape[0]):
        total = total + got_ref[p]
    z_ref[...] = total + d_ref[...] * x_ref[...]


def call(kernel, out, inputs, scratch=(), specs=None, out_specs=None, flops=2_000_000):
    return pl.pallas_call(
        kernel,
        out_shape=out,
        in_specs=specs or [VMEM] * len(inputs),
        out_specs=out_specs or jax.tree.map(lambda _: VMEM, out),
        scratch_shapes=list(scratch),
        cost_estimate=pl.CostEstimate(flops=flops, bytes_accessed=100_000, transcendentals=0),
        compiler_params=pltpu.CompilerParams(vmem_limit_bytes=24 << 20),
    )(*inputs)


def shards(couplings, diag_terms, start_block):
    cols = lax.axis_size("col")
    rows = lax.axis_size("row")
    swap = [(i, i ^ 1) for i in range(cols)]
    whole, part, rest = (2 * W, W), (CHUNK, W), (2 * W - CHUNK, W)
    tall = pltpu.VMEM((8, 2 * W), F32)
    short = pltpu.VMEM((8, W), F32)
    flat = in_vmem((1, FLAT))

    def exchanged(block, axis):
        return lax.all_to_all(block, axis, 0, 0, tiled=True)

    mark = call(opening_kernel, in_vmem((8, 128)), (), flops=5_000_000_000)
    held, mark = lax.optimization_barrier((start_block, mark))
    cross = lax.ppermute(held, "col", swap)
    sent, x, d, high, near, far = call(
        first_kernel,
        (in_vmem((cols, 1, FLAT)), flat, flat, in_vmem(whole, BF16), in_vmem(part, BF16), in_vmem(rest, BF16)),
        (start_block, diag_terms, couplings, mark),
        [short, tall],
    )
    got = exchanged(sent, "col")
    total = call(sum_kernel, flat, (got,))
    many = in_vmem((8, 2 * W))
    sent, x_rows = call(
        first_backward_kernel, (in_vmem((rows, 1, FLAT)), many), (got, x, cross, total, high, near, far)
    )
    got = exchanged(sent, "row")
    z = call(collect_kernel, flat, (got, d, x))
    sent = call(
        forward_kernel,
        pltpu.HBM((cols, 1, FLAT), F32),
        (z, x, high, near, far),
        [pltpu.VMEM((cols, 1, FLAT), F32), pltpu.VMEM((2, 1, FLAT), F32), short, tall, pltpu.SemaphoreType.DMA((2,))],
        out_specs=HBM,
    )
    cross = lax.ppermute(z, "col", swap)
    got = exchanged(sent, "col")
    sent = call(
        second_backward_kernel,
        in_vmem((rows, 1, FLAT + 128)),
        (got, z, cross, x_rows, high, near, pltpu.with_memory_space_constraint(far, pltpu.HBM)),
        [
            pltpu.VMEM(rest, BF16),
            tall,
            pltpu.VMEM((1, FLAT), F32),
            pltpu.VMEM((1, 128), F32),
            pltpu.VMEM((24, W), F32),
            pltpu.SemaphoreType.DMA((2 * W // CHUNK - 1,)),
        ],
        [VMEM] * 6 + [HBM],
    )
    got = exchanged(sent, "row")
    sent, basis, coef = call(
        residual_kernel,
        (in_vmem((cols, 1, 128)), in_vmem((16, W)), in_vmem((40, 128))),
        (got, z, x, d),
    )
    got = exchanged(sent, "col")
    f32 = lambda *shape: jax.ShapeDtypeStruct(shape, F32)
    blocks, coeffs = call(last_kernel, (f32(3, 2, W), f32(2, 3, 2, 3)), (got, basis, coef))
    return jnp.swapaxes(blocks, 0, 1), jnp.swapaxes(coeffs, 1, 2)


def solution(mesh):
    placed = (P("row", "col"), P("col"), P(None, "col"))
    return jax.shard_map(
        shards, mesh=mesh, in_specs=placed, out_specs=(P(None, None, "col"), P()), check_vma=False
    )
```

```python
import jax
import jax.numpy as jnp
from jax import lax
from jax.experimental import pallas as pl
from jax.experimental.pallas import tpu as pltpu
from jax.sharding import PartitionSpec as P


M = 24576
SHIFT = 2.5
W = 768
FLAT = 3 * W
CHUNK = 512
STRIP = 16
F32 = jnp.float32
BF16 = jnp.bfloat16
VMEM = pl.BlockSpec(memory_space=pltpu.VMEM)
HBM = pl.BlockSpec(memory_space=pltpu.HBM)


def in_vmem(shape, dtype=F32):
    return pltpu.VMEM(shape, dtype)


def three_parts(x):
    first = x.astype(BF16).astype(F32)
    rest = x - first
    second = rest.astype(BF16).astype(F32)
    return jnp.concatenate([first, second, rest - second], 0).astype(BF16)


def folded(wide):
    return wide[0:8] + wide[8:16] + wide[16:24]


def over_rows(parts, matrix):
    return lax.dot_general(parts, matrix, (((1,), (1,)), ((), ())), preferred_element_type=F32)


def over_cols(parts, matrix):
    return lax.dot_general(parts, matrix, (((1,), (0,)), ((), ())), preferred_element_type=F32)


def rows_of(flat):
    return [flat[:, k * W : (k + 1) * W] for k in range(3)]


def inner(a, b):
    return jnp.sum(a * b, axis=1, keepdims=True)


def packed(values):
    lane = lax.broadcasted_iota(jnp.int32, (1, 128), 1)
    tile = jnp.zeros((1, 128), F32)
    for at, value in enumerate(values):
        tile = jnp.where(lane == at, value, tile)
    return tile


def products_of(rows):
    return [sum(inner(a, b) for a, b in zip(rows[i], rows[j])) for i in range(6) for j in range(i, 6)]


def unpacked(tile, count):
    lane = lax.broadcasted_iota(jnp.int32, (1, 128), 1)
    return [jnp.sum(jnp.where(lane == at, tile, 0.0), axis=1, keepdims=True) for at in range(count)]


def symmetric(six):
    a, b, c, d, e, f = six
    return [[a, b, c], [b, d, e], [c, e, f]]


def times(a, b):
    return [[sum(a[i][k] * b[k][j] for k in range(3)) for j in range(3)] for i in range(3)]


def turned(a):
    return [[a[j][i] for j in range(3)] for i in range(3)]


def minus(a, b):
    return [[a[i][j] - b[i][j] for j in range(3)] for i in range(3)]


def cholesky(h):
    zero = jnp.zeros_like(h[0][0])
    a = jnp.sqrt(h[0][0])
    b = h[1][0] / a
    c = h[2][0] / a
    d = jnp.sqrt(h[1][1] - b * b)
    e = (h[2][1] - c * b) / d
    f = jnp.sqrt(h[2][2] - c * c - e * e)
    return [[a, zero, zero], [b, d, zero], [c, e, f]]


def inverse(low):
    zero = jnp.zeros_like(low[0][0])
    a, d, f = 1.0 / low[0][0], 1.0 / low[1][1], 1.0 / low[2][2]
    b = -low[1][0] * a * d
    e = -low[2][1] * d * f
    c = -(low[2][0] * a + low[2][1] * b) * f
    return [[a, zero, zero], [b, d, zero], [c, e, f]]


def combine(matrix, vectors):
    return [sum(matrix[i][k] * vectors[k] for k in range(3)) for i in range(3)]


def place(row_index, forward_ref, sent_ref):
    for half in range(2):
        for k in range(3):
            sent_ref[2 * row_index + half, :, k * W : (k + 1) * W] = forward_ref[k : k + 1, half * W : (half + 1) * W]


def opening_kernel(mark_ref):
    mark_ref[...] = jnp.zeros_like(mark_ref)


def first_kernel(x_ref, d_ref, a_ref, mark_ref, sent_ref, flat_ref, diag_ref, high_ref, near_ref, far_ref, x_rows, forward):
    row_index = lax.axis_index("row")
    x_rows[...] = jnp.zeros_like(x_rows)
    x_rows[0:3, :] = x_ref[...]
    for k in range(3):
        lanes = slice(k * W, (k + 1) * W)
        flat_ref[:, lanes] = x_ref[k : k + 1, :]
        diag_ref[:, lanes] = d_ref[...].reshape(1, W) - SHIFT
    x = flat_ref[...]
    for p in range(sent_ref.shape[0]):
        sent_ref[p] = x
    parts = three_parts(x_rows[...])
    for start in range(0, 2 * W, CHUNK):
        piece = slice(start, start + CHUNK)
        low_ref, base = (near_ref, 0) if start == 0 else (far_ref, CHUNK)
        for at in range(start, start + CHUNK, STRIP):
            block = a_ref[at : at + STRIP, :]
            high = block.astype(BF16)
            high_ref[at : at + STRIP, :] = high
            low_ref[at - base : at - base + STRIP, :] = (block - high.astype(F32)).astype(BF16)
        low = low_ref[start - base : start - base + CHUNK, :]
        wide = over_rows(parts, high_ref[piece, :]) + over_rows(parts, low)
        forward[:, piece] = 0.5 * folded(wide)
    place(row_index, forward, sent_ref)


def forward_kernel(z_ref, x_ref, high_ref, near_ref, far_ref, sent_ref, z_rows, forward):
    row_index = lax.axis_index("row")
    home = lax.axis_index("col") // 2 == row_index
    z = z_ref[...]
    z_rows[...] = jnp.zeros_like(z_rows)
    for k, row in enumerate(rows_of(z)):
        z_rows[k : k + 1, :] = row
    parts = three_parts(z_rows[...])
    six = rows_of(x_ref[...]) + rows_of(z)
    tile = packed(products_of([[row] for row in six]))
    head = jnp.where(home, z[:, 0:128], tile)
    for p in range(sent_ref.shape[0]):
        sent_ref[p, :, 0:128] = head
        sent_ref[p, :, 128:] = z[:, 128:]
    low = jnp.concatenate([over_rows(parts, near_ref[...]), over_rows(parts, far_ref[...])], 1)
    forward[...] = 0.5 * folded(over_rows(parts, high_ref[...]) + low)
    place(row_index, forward, sent_ref)


def first_backward_kernel(got_ref, own_ref, cross_ref, total_ref, high_ref, near_ref, far_ref, sent_ref, v_rows):
    assemble(got_ref, own_ref, cross_ref, v_rows)
    parts = three_parts(v_rows[...])
    wide = over_cols(parts, high_ref[...]) + over_cols(parts[:, :CHUNK], near_ref[...])
    wide = wide + over_cols(parts[:, CHUNK:], far_ref[...])
    deliver(0.5 * folded(wide), rows_of(total_ref[...]), sent_ref)


def second_backward_kernel(
    got_ref, own_ref, cross_ref, x_rows, high_ref, near_ref, far_hbm, sent_ref, far, v_rows, total_ref, tile_ref, wide_ref, sems
):
    pieces = [slice(start, start + CHUNK) for start in range(0, far.shape[0], CHUNK)]
    copies = [pltpu.make_async_copy(far_hbm.at[piece], far.at[piece], sems.at[i]) for i, piece in enumerate(pieces)]
    for copy in copies:
        copy.start()
    assemble(got_ref, own_ref, cross_ref, v_rows)
    parts = three_parts(v_rows[...])
    wide_ref[...] = over_cols(parts, high_ref[...]) + over_cols(parts[:, :CHUNK], near_ref[...])
    gram_kernel(got_ref, x_rows, total_ref, tile_ref)
    for p in range(sent_ref.shape[0]):
        sent_ref[p, :, FLAT:] = tile_ref[...]
    total = rows_of(total_ref[...])
    wide = wide_ref[...]
    for copy, piece in zip(copies, pieces):
        copy.wait()
        wide = wide + over_cols(parts[:, CHUNK + piece.start : CHUNK + piece.stop], far[piece, :])
    deliver(0.5 * folded(wide), total, sent_ref)


def deliver(back, total, sent_ref):
    for k in range(3):
        part = back[k : k + 1] + total[k]
        for p in range(sent_ref.shape[0]):
            sent_ref[p, :, k * W : (k + 1) * W] = part


def assemble(got_ref, own_ref, cross_ref, v_rows):
    row_index = lax.axis_index("row")
    col_index = lax.axis_index("col")
    home = col_index // 2 == row_index
    v_rows[...] = jnp.zeros_like(v_rows)
    own = rows_of(own_ref[...])
    cross = rows_of(cross_ref[...]) if cross_ref.shape[0] == 1 else [cross_ref[k : k + 1, :] for k in range(3)]
    for half in range(2):
        sent_here = rows_of(got_ref[2 * row_index + half])
        for k in range(3):
            mine = jnp.where(col_index % 2 == half, own[k], cross[k])
            v_rows[k : k + 1, half * W : (half + 1) * W] = jnp.where(home, mine, sent_here[k])


def sum_kernel(got_ref, total_ref):
    home = lax.axis_index("col") // 2 == lax.axis_index("row")
    total = got_ref[0]
    for p in range(1, got_ref.shape[0]):
        total = total + got_ref[p]
    total_ref[...] = jnp.where(home, total, 0.0)


def gram_kernel(got_ref, x_rows, total_ref, tile_ref):
    sum_kernel(got_ref, total_ref)
    row_index = lax.axis_index("row")
    tile = jnp.zeros((1, 128), F32)
    for p in range(got_ref.shape[0]):
        tile = tile + jnp.where(row_index == p // 2, 0.0, got_ref[p, :, 0:128])
    z = [rows_of(got_ref[2 * row_index + half]) for half in range(2)]
    rows = [[x_rows[k : k + 1, half * W : (half + 1) * W] for half in range(2)] for k in range(3)]
    rows += [[z[half][k] for half in range(2)] for k in range(3)]
    tile_ref[...] = tile + packed(products_of(rows))


def algebra(tile, coef_ref):
    flat = iter(unpacked(tile, 21))
    gram = {(i, j): next(flat) for i in range(6) for j in range(i, 6)}
    g00 = symmetric([gram[i, j] for i in range(3) for j in range(i, 3)])
    g01 = [[gram[i, j + 3] for j in range(3)] for i in range(3)]
    g11 = symmetric([gram[i + 3, j + 3] for i in range(3) for j in range(i, 3)])
    n0 = inverse(cholesky(g00))
    n0t = turned(n0)
    c0 = times(times(n0, turned(g01)), n0t)
    l1 = cholesky(minus(times(times(n0, g11), n0t), times(c0, turned(c0))))
    n1 = inverse(l1)
    at = 0
    for matrix in (n0, n1, c0, l1):
        for i in range(3):
            for j in range(3):
                coef_ref[at : at + 1, :] = jnp.broadcast_to(matrix[i][j], (1, 128))
                at += 1


def loaded(coef_ref, which, width):
    row = lambda at: coef_ref[at : at + 1, :]
    wide = lambda v: v if width == 128 else jnp.concatenate([v] * (width // 128), 1)
    return [[wide(row(9 * which + 3 * i + j)) for j in range(3)] for i in range(3)]


def residual_kernel(got_ref, z_ref, x_ref, d_ref, sent_ref, basis_ref, coef_ref):
    away = (lax.axis_index("col") // 2 + 1) % got_ref.shape[0]
    algebra(got_ref[away, :, FLAT:], coef_ref)
    total = got_ref[0, :, 0:FLAT]
    for p in range(1, got_ref.shape[0]):
        total = total + got_ref[p, :, 0:FLAT]
    z = z_ref[...]
    y = rows_of(total + d_ref[...] * z)
    n0, n1, c0, l1 = (loaded(coef_ref, i, W) for i in range(4))
    q0 = combine(n0, rows_of(x_ref[...]))
    u = combine(n0, rows_of(z))
    q1 = combine(n1, [a - b for a, b in zip(u, combine(c0, q0))])
    w = combine(n1, [a - b for a, b in zip(combine(n0, y), combine(c0, u))])
    known = [a + b for a, b in zip(combine(turned(l1), q0), combine(c0, q1))]
    w = [a - b for a, b in zip(w, known)]
    values = [inner(a, b) for a in w for b in q0 + q1]
    values += [inner(w[i], w[j]) for i in range(3) for j in range(i, 3)]
    tile = packed(values)
    for p in range(sent_ref.shape[0]):
        sent_ref[p] = tile
    for at, row in enumerate(q0 + q1 + w):
        basis_ref[at : at + 1, :] = row


def last_kernel(got_ref, basis_ref, coef_ref, out_ref, coeffs_ref):
    tile = got_ref[0]
    for p in range(1, got_ref.shape[0]):
        tile = tile + got_ref[p]
    values = unpacked(tile, 24)
    d0 = [values[6 * i : 6 * i + 3] for i in range(3)]
    d1 = [values[6 * i + 3 : 6 * i + 6] for i in range(3)]
    h2 = minus(minus(symmetric(values[18:]), times(d0, turned(d0))), times(d1, turned(d1)))
    l2 = cholesky(h2)
    n2 = inverse(l2)
    rows = [basis_ref[at : at + 1, :] for at in range(9)]
    q0, q1, w = rows[:3], rows[3:6], rows[6:]
    known = [a + b for a, b in zip(combine(d0, q0), combine(d1, q1))]
    q2 = combine(n2, [a - b for a, b in zip(w, known)])
    root = float(M) ** 0.5
    for k in range(3):
        out_ref[k, 0:1, :] = q1[k] * root
        out_ref[k, 1:2, :] = q2[k] * root
    c0, l1 = ([[v[:, 0:1] for v in line] for line in loaded(coef_ref, i, 128)] for i in (2, 3))
    down = lax.broadcasted_iota(jnp.int32, (3, 3), 0)
    across = lax.broadcasted_iota(jnp.int32, (3, 3), 1)

    def square(matrix, shift):
        tile = jnp.where(down == across, shift, 0.0)
        for i in range(3):
            for j in range(3):
                tile = jnp.where((down == i) & (across == j), tile + matrix[i][j], tile)
        return tile

    second = [[c0[i][j] + d1[i][j] for j in range(3)] for i in range(3)]
    blocks = [[square(c0, SHIFT), square(l1, 0.0)], [square(second, SHIFT), square(l2, 0.0)]]
    for j in range(2):
        for i in range(3):
            for which in range(2):
                coeffs_ref[j, i, which : which + 1, :] = blocks[j][which][i : i + 1, :]


def collect_kernel(got_ref, d_ref, x_ref, z_ref):
    total = got_ref[0]
    for p in range(1, got_ref.shape[0]):
        total = total + got_ref[p]
    z_ref[...] = total + d_ref[...] * x_ref[...]


def call(kernel, out, inputs, scratch=(), specs=None, out_specs=None, flops=2_000_000):
    return pl.pallas_call(
        kernel,
        out_shape=out,
        in_specs=specs or [VMEM] * len(inputs),
        out_specs=out_specs or jax.tree.map(lambda _: VMEM, out),
        scratch_shapes=list(scratch),
        cost_estimate=pl.CostEstimate(flops=flops, bytes_accessed=100_000, transcendentals=0),
        compiler_params=pltpu.CompilerParams(vmem_limit_bytes=24 << 20),
    )(*inputs)


def shards(couplings, diag_terms, start_block):
    cols = lax.axis_size("col")
    rows = lax.axis_size("row")
    swap = [(i, i ^ 1) for i in range(cols)]
    whole, part, rest = (2 * W, W), (CHUNK, W), (2 * W - CHUNK, W)
    tall = pltpu.VMEM((8, 2 * W), F32)
    short = pltpu.VMEM((8, W), F32)
    flat = in_vmem((1, FLAT))

    def exchanged(block, axis):
        return lax.all_to_all(block, axis, 0, 0, tiled=True)

    mark = call(opening_kernel, in_vmem((8, 128)), (), flops=5_000_000_000)
    held, mark = lax.optimization_barrier((start_block, mark))
    cross = lax.ppermute(held, "col", swap)
    sent, x, d, high, near, far = call(
        first_kernel,
        (in_vmem((cols, 1, FLAT)), flat, flat, in_vmem(whole, BF16), in_vmem(part, BF16), in_vmem(rest, BF16)),
        (start_block, diag_terms, couplings, mark),
        [short, tall],
    )
    got = exchanged(sent, "col")
    total = call(sum_kernel, flat, (got,))
    many = in_vmem((8, 2 * W))
    sent, x_rows = call(
        first_backward_kernel, (in_vmem((rows, 1, FLAT)), many), (got, x, cross, total, high, near, far)
    )
    got = exchanged(sent, "row")
    z = call(collect_kernel, flat, (got, d, x))
    slots = pltpu.HBM((cols, 1, FLAT), F32)
    sent = call(forward_kernel, slots, (z, x, high, near, far), [short, tall], out_specs=pl.BlockSpec())
    cross = lax.ppermute(z, "col", swap)
    got = exchanged(sent, "col")
    sent = call(
        second_backward_kernel,
        in_vmem((rows, 1, FLAT + 128)),
        (got, z, cross, x_rows, high, near, pltpu.with_memory_space_constraint(far, pltpu.HBM)),
        [
            pltpu.VMEM(rest, BF16),
            tall,
            pltpu.VMEM((1, FLAT), F32),
            pltpu.VMEM((1, 128), F32),
            pltpu.VMEM((24, W), F32),
            pltpu.SemaphoreType.DMA((2 * W // CHUNK - 1,)),
        ],
        [VMEM] * 6 + [HBM],
    )
    got = exchanged(sent, "row")
    sent, basis, coef = call(
        residual_kernel,
        (in_vmem((cols, 1, 128)), in_vmem((16, W)), in_vmem((40, 128))),
        (got, z, x, d),
    )
    got = exchanged(sent, "col")
    f32 = lambda *shape: jax.ShapeDtypeStruct(shape, F32)
    blocks, coeffs = call(last_kernel, (f32(3, 2, W), f32(2, 3, 2, 3)), (got, basis, coef))
    return jnp.swapaxes(blocks, 0, 1), jnp.swapaxes(coeffs, 1, 2)


def solution(mesh):
    placed = (P("row", "col"), P("col"), P(None, "col"))
    return jax.shard_map(
        shards, mesh=mesh, in_specs=placed, out_specs=(P(None, None, "col"), P()), check_vma=False
    )
```

```python
import jax
import jax.numpy as jnp
from jax import lax
from jax.experimental import pallas as pl
from jax.experimental.pallas import tpu as pltpu
from jax.sharding import PartitionSpec as P


M = 24576
SHIFT = 2.5
W = 768
FLAT = 3 * W
CHUNK = 512
STRIP = 16
F32 = jnp.float32
BF16 = jnp.bfloat16
VMEM = pl.BlockSpec(memory_space=pltpu.VMEM)
HBM = pl.BlockSpec(memory_space=pltpu.HBM)


def in_vmem(shape, dtype=F32):
    return pltpu.VMEM(shape, dtype)


def three_parts(x):
    first = x.astype(BF16).astype(F32)
    rest = x - first
    second = rest.astype(BF16).astype(F32)
    return jnp.concatenate([first, second, rest - second], 0).astype(BF16)


def folded(wide):
    return wide[0:8] + wide[8:16] + wide[16:24]


def over_rows(parts, matrix):
    return lax.dot_general(parts, matrix, (((1,), (1,)), ((), ())), preferred_element_type=F32)


def over_cols(parts, matrix):
    return lax.dot_general(parts, matrix, (((1,), (0,)), ((), ())), preferred_element_type=F32)


def rows_of(flat):
    return [flat[:, k * W : (k + 1) * W] for k in range(3)]


def inner(a, b):
    return jnp.sum(a * b, axis=1, keepdims=True)


def packed(values):
    lane = lax.broadcasted_iota(jnp.int32, (1, 128), 1)
    tile = jnp.zeros((1, 128), F32)
    for at, value in enumerate(values):
        tile = jnp.where(lane == at, value, tile)
    return tile


def products_of(rows):
    return [sum(inner(a, b) for a, b in zip(rows[i], rows[j])) for i in range(6) for j in range(i, 6)]


def unpacked(tile, count):
    lane = lax.broadcasted_iota(jnp.int32, (1, 128), 1)
    return [jnp.sum(jnp.where(lane == at, tile, 0.0), axis=1, keepdims=True) for at in range(count)]


def symmetric(six):
    a, b, c, d, e, f = six
    return [[a, b, c], [b, d, e], [c, e, f]]


def times(a, b):
    return [[sum(a[i][k] * b[k][j] for k in range(3)) for j in range(3)] for i in range(3)]


def turned(a):
    return [[a[j][i] for j in range(3)] for i in range(3)]


def minus(a, b):
    return [[a[i][j] - b[i][j] for j in range(3)] for i in range(3)]


def cholesky(h):
    zero = jnp.zeros_like(h[0][0])
    a = jnp.sqrt(h[0][0])
    b = h[1][0] / a
    c = h[2][0] / a
    d = jnp.sqrt(h[1][1] - b * b)
    e = (h[2][1] - c * b) / d
    f = jnp.sqrt(h[2][2] - c * c - e * e)
    return [[a, zero, zero], [b, d, zero], [c, e, f]]


def inverse(low):
    zero = jnp.zeros_like(low[0][0])
    a, d, f = 1.0 / low[0][0], 1.0 / low[1][1], 1.0 / low[2][2]
    b = -low[1][0] * a * d
    e = -low[2][1] * d * f
    c = -(low[2][0] * a + low[2][1] * b) * f
    return [[a, zero, zero], [b, d, zero], [c, e, f]]


def combine(matrix, vectors):
    return [sum(matrix[i][k] * vectors[k] for k in range(3)) for i in range(3)]


def place(row_index, forward_ref, sent_ref):
    for half in range(2):
        for k in range(3):
            sent_ref[2 * row_index + half, :, k * W : (k + 1) * W] = forward_ref[k : k + 1, half * W : (half + 1) * W]


def opening_kernel(mark_ref):
    mark_ref[...] = jnp.zeros_like(mark_ref)


def first_kernel(x_ref, d_ref, a_ref, mark_ref, sent_ref, flat_ref, diag_ref, high_ref, low_ref, x_rows, forward):
    row_index = lax.axis_index("row")
    x_rows[...] = jnp.zeros_like(x_rows)
    x_rows[0:3, :] = x_ref[...]
    for k in range(3):
        lanes = slice(k * W, (k + 1) * W)
        flat_ref[:, lanes] = x_ref[k : k + 1, :]
        diag_ref[:, lanes] = d_ref[...].reshape(1, W) - SHIFT
    x = flat_ref[...]
    for p in range(sent_ref.shape[0]):
        sent_ref[p] = x
    parts = three_parts(x_rows[...])
    for start in range(0, 2 * W, CHUNK):
        piece = slice(start, start + CHUNK)
        for at in range(start, start + CHUNK, STRIP):
            strip = slice(at, at + STRIP)
            block = a_ref[strip, :]
            high = block.astype(BF16)
            high_ref[strip, :] = high
            low_ref[strip, :] = (block - high.astype(F32)).astype(BF16)
        wide = over_rows(parts, high_ref[piece, :]) + over_rows(parts, low_ref[piece, :])
        forward[:, piece] = 0.5 * folded(wide)
    place(row_index, forward, sent_ref)


def forward_kernel(z_ref, x_ref, high_ref, low_ref, sent_ref, z_rows, forward):
    row_index = lax.axis_index("row")
    home = lax.axis_index("col") // 2 == row_index
    z = z_ref[...]
    z_rows[...] = jnp.zeros_like(z_rows)
    for k, row in enumerate(rows_of(z)):
        z_rows[k : k + 1, :] = row
    parts = three_parts(z_rows[...])
    six = rows_of(x_ref[...]) + rows_of(z)
    tile = packed(products_of([[row] for row in six]))
    head = jnp.where(home, z[:, 0:128], tile)
    for p in range(sent_ref.shape[0]):
        sent_ref[p, :, 0:128] = head
        sent_ref[p, :, 128:] = z[:, 128:]
    cut = 4 * W // 3
    tall = over_rows(high_ref[cut:, :], parts) + over_rows(low_ref[cut:, :], parts)
    wide = over_rows(parts, high_ref[0:cut, :]) + over_rows(parts, low_ref[0:cut, :])
    forward[:, 0:cut] = 0.5 * folded(wide)
    forward[:, cut:] = 0.5 * folded(tall.T)
    place(row_index, forward, sent_ref)


def first_backward_kernel(got_ref, own_ref, cross_ref, total_ref, high_ref, low_ref, sent_ref, v_rows):
    backward(got_ref, own_ref, cross_ref, total_ref, high_ref, low_ref, sent_ref, v_rows)


def second_backward_kernel(
    got_ref, own_ref, cross_ref, x_rows, high_ref, low_hbm, sent_ref, low, v_rows, total_ref, tile_ref, wide_ref, sems
):
    pieces = [slice(start, start + CHUNK) for start in range(0, 2 * W, CHUNK)]
    copies = [pltpu.make_async_copy(low_hbm.at[piece], low.at[piece], sems.at[i]) for i, piece in enumerate(pieces)]
    for copy in copies:
        copy.start()
    assemble(got_ref, own_ref, cross_ref, v_rows)
    parts = three_parts(v_rows[...])
    wide_ref[...] = over_cols(parts, high_ref[...])
    gram_kernel(got_ref, x_rows, total_ref, tile_ref)
    for p in range(sent_ref.shape[0]):
        sent_ref[p, :, FLAT:] = tile_ref[...]
    total = rows_of(total_ref[...])
    wide = wide_ref[...]
    for copy, piece in zip(copies, pieces):
        copy.wait()
        wide = wide + over_cols(parts[:, piece], low[piece, :])
    deliver(0.5 * folded(wide), total, sent_ref)


def backward(got_ref, own_ref, cross_ref, total_ref, high_ref, low_ref, sent_ref, v_rows):
    assemble(got_ref, own_ref, cross_ref, v_rows)
    parts = three_parts(v_rows[...])
    wide = over_cols(parts, high_ref[...]) + over_cols(parts, low_ref[...])
    deliver(0.5 * folded(wide), rows_of(total_ref[...]), sent_ref)


def deliver(back, total, sent_ref):
    for k in range(3):
        part = back[k : k + 1] + total[k]
        for p in range(sent_ref.shape[0]):
            sent_ref[p, :, k * W : (k + 1) * W] = part


def assemble(got_ref, own_ref, cross_ref, v_rows):
    row_index = lax.axis_index("row")
    col_index = lax.axis_index("col")
    home = col_index // 2 == row_index
    v_rows[...] = jnp.zeros_like(v_rows)
    own = rows_of(own_ref[...])
    cross = rows_of(cross_ref[...]) if cross_ref.shape[0] == 1 else [cross_ref[k : k + 1, :] for k in range(3)]
    for half in range(2):
        sent_here = rows_of(got_ref[2 * row_index + half])
        for k in range(3):
            mine = jnp.where(col_index % 2 == half, own[k], cross[k])
            v_rows[k : k + 1, half * W : (half + 1) * W] = jnp.where(home, mine, sent_here[k])


def sum_kernel(got_ref, total_ref):
    home = lax.axis_index("col") // 2 == lax.axis_index("row")
    total = got_ref[0]
    for p in range(1, got_ref.shape[0]):
        total = total + got_ref[p]
    total_ref[...] = jnp.where(home, total, 0.0)


def gram_kernel(got_ref, x_rows, total_ref, tile_ref):
    sum_kernel(got_ref, total_ref)
    row_index = lax.axis_index("row")
    tile = jnp.zeros((1, 128), F32)
    for p in range(got_ref.shape[0]):
        tile = tile + jnp.where(row_index == p // 2, 0.0, got_ref[p, :, 0:128])
    z = [rows_of(got_ref[2 * row_index + half]) for half in range(2)]
    rows = [[x_rows[k : k + 1, half * W : (half + 1) * W] for half in range(2)] for k in range(3)]
    rows += [[z[half][k] for half in range(2)] for k in range(3)]
    tile_ref[...] = tile + packed(products_of(rows))


def algebra(tile, coef_ref):
    flat = iter(unpacked(tile, 21))
    gram = {(i, j): next(flat) for i in range(6) for j in range(i, 6)}
    g00 = symmetric([gram[i, j] for i in range(3) for j in range(i, 3)])
    g01 = [[gram[i, j + 3] for j in range(3)] for i in range(3)]
    g11 = symmetric([gram[i + 3, j + 3] for i in range(3) for j in range(i, 3)])
    n0 = inverse(cholesky(g00))
    n0t = turned(n0)
    c0 = times(times(n0, turned(g01)), n0t)
    l1 = cholesky(minus(times(times(n0, g11), n0t), times(c0, turned(c0))))
    n1 = inverse(l1)
    at = 0
    for matrix in (n0, n1, c0, l1):
        for i in range(3):
            for j in range(3):
                coef_ref[at : at + 1, :] = jnp.broadcast_to(matrix[i][j], (1, 128))
                at += 1


def loaded(coef_ref, which, width):
    row = lambda at: coef_ref[at : at + 1, :]
    wide = lambda v: v if width == 128 else jnp.concatenate([v] * (width // 128), 1)
    return [[wide(row(9 * which + 3 * i + j)) for j in range(3)] for i in range(3)]


def residual_kernel(got_ref, z_ref, x_ref, d_ref, sent_ref, basis_ref, coef_ref):
    away = (lax.axis_index("col") // 2 + 1) % got_ref.shape[0]
    algebra(got_ref[away, :, FLAT:], coef_ref)
    total = got_ref[0, :, 0:FLAT]
    for p in range(1, got_ref.shape[0]):
        total = total + got_ref[p, :, 0:FLAT]
    z = z_ref[...]
    y = rows_of(total + d_ref[...] * z)
    n0, n1, c0, l1 = (loaded(coef_ref, i, W) for i in range(4))
    q0 = combine(n0, rows_of(x_ref[...]))
    u = combine(n0, rows_of(z))
    q1 = combine(n1, [a - b for a, b in zip(u, combine(c0, q0))])
    w = combine(n1, [a - b for a, b in zip(combine(n0, y), combine(c0, u))])
    known = [a + b for a, b in zip(combine(turned(l1), q0), combine(c0, q1))]
    w = [a - b for a, b in zip(w, known)]
    values = [inner(a, b) for a in w for b in q0 + q1]
    values += [inner(w[i], w[j]) for i in range(3) for j in range(i, 3)]
    tile = packed(values)
    for p in range(sent_ref.shape[0]):
        sent_ref[p] = tile
    for at, row in enumerate(q0 + q1 + w):
        basis_ref[at : at + 1, :] = row


def last_kernel(got_ref, basis_ref, coef_ref, out_ref, coeffs_ref):
    tile = got_ref[0]
    for p in range(1, got_ref.shape[0]):
        tile = tile + got_ref[p]
    values = unpacked(tile, 24)
    d0 = [values[6 * i : 6 * i + 3] for i in range(3)]
    d1 = [values[6 * i + 3 : 6 * i + 6] for i in range(3)]
    h2 = minus(minus(symmetric(values[18:]), times(d0, turned(d0))), times(d1, turned(d1)))
    l2 = cholesky(h2)
    n2 = inverse(l2)
    rows = [basis_ref[at : at + 1, :] for at in range(9)]
    q0, q1, w = rows[:3], rows[3:6], rows[6:]
    known = [a + b for a, b in zip(combine(d0, q0), combine(d1, q1))]
    q2 = combine(n2, [a - b for a, b in zip(w, known)])
    root = float(M) ** 0.5
    for k in range(3):
        out_ref[k, 0:1, :] = q1[k] * root
        out_ref[k, 1:2, :] = q2[k] * root
    c0, l1 = ([[v[:, 0:1] for v in line] for line in loaded(coef_ref, i, 128)] for i in (2, 3))
    down = lax.broadcasted_iota(jnp.int32, (3, 3), 0)
    across = lax.broadcasted_iota(jnp.int32, (3, 3), 1)

    def square(matrix, shift):
        tile = jnp.where(down == across, shift, 0.0)
        for i in range(3):
            for j in range(3):
                tile = jnp.where((down == i) & (across == j), tile + matrix[i][j], tile)
        return tile

    second = [[c0[i][j] + d1[i][j] for j in range(3)] for i in range(3)]
    blocks = [[square(c0, SHIFT), square(l1, 0.0)], [square(second, SHIFT), square(l2, 0.0)]]
    for j in range(2):
        for i in range(3):
            for which in range(2):
                coeffs_ref[j, i, which : which + 1, :] = blocks[j][which][i : i + 1, :]


def collect_kernel(got_ref, d_ref, x_ref, z_ref):
    total = got_ref[0]
    for p in range(1, got_ref.shape[0]):
        total = total + got_ref[p]
    z_ref[...] = total + d_ref[...] * x_ref[...]


def call(kernel, out, inputs, scratch=(), specs=None, out_specs=None, flops=2_000_000):
    return pl.pallas_call(
        kernel,
        out_shape=out,
        in_specs=specs or [VMEM] * len(inputs),
        out_specs=out_specs or jax.tree.map(lambda _: VMEM, out),
        scratch_shapes=list(scratch),
        cost_estimate=pl.CostEstimate(flops=flops, bytes_accessed=100_000, transcendentals=0),
        compiler_params=pltpu.CompilerParams(vmem_limit_bytes=24 << 20),
    )(*inputs)


def shards(couplings, diag_terms, start_block):
    cols = lax.axis_size("col")
    rows = lax.axis_size("row")
    swap = [(i, i ^ 1) for i in range(cols)]
    whole = (2 * W, W)
    tall = pltpu.VMEM((8, 2 * W), F32)
    short = pltpu.VMEM((8, W), F32)
    flat = in_vmem((1, FLAT))

    def exchanged(block, axis):
        return lax.all_to_all(block, axis, 0, 0, tiled=True)

    mark = call(opening_kernel, in_vmem((8, 128)), (), flops=5_000_000_000)
    held, mark = lax.optimization_barrier((start_block, mark))
    cross = lax.ppermute(held, "col", swap)
    sent, x, d, high, low = call(
        first_kernel,
        (in_vmem((cols, 1, FLAT)), flat, flat, in_vmem(whole, BF16), in_vmem(whole, BF16)),
        (start_block, diag_terms, couplings, mark),
        [short, tall],
    )
    got = exchanged(sent, "col")
    total = call(sum_kernel, flat, (got,))
    many = in_vmem((8, 2 * W))
    sent, x_rows = call(
        first_backward_kernel, (in_vmem((rows, 1, FLAT)), many), (got, x, cross, total, high, low)
    )
    got = exchanged(sent, "row")
    z = call(collect_kernel, flat, (got, d, x))
    slots = jax.ShapeDtypeStruct((cols, 1, FLAT), F32)
    sent = call(forward_kernel, slots, (z, x, high, low), [short, tall])
    cross = lax.ppermute(z, "col", swap)
    got = exchanged(sent, "col")
    sent = call(
        second_backward_kernel,
        in_vmem((rows, 1, FLAT + 128)),
        (got, z, cross, x_rows, high, pltpu.with_memory_space_constraint(low, pltpu.HBM)),
        [
            pltpu.VMEM(whole, BF16),
            tall,
            pltpu.VMEM((1, FLAT), F32),
            pltpu.VMEM((1, 128), F32),
            pltpu.VMEM((24, W), F32),
            pltpu.SemaphoreType.DMA((2 * W // CHUNK,)),
        ],
        [VMEM] * 5 + [HBM],
    )
    got = exchanged(sent, "row")
    sent, basis, coef = call(
        residual_kernel,
        (in_vmem((cols, 1, 128)), in_vmem((16, W)), in_vmem((40, 128))),
        (got, z, x, d),
    )
    got = exchanged(sent, "col")
    f32 = lambda *shape: jax.ShapeDtypeStruct(shape, F32)
    blocks, coeffs = call(last_kernel, (f32(3, 2, W), f32(2, 3, 2, 3)), (got, basis, coef))
    return jnp.swapaxes(blocks, 0, 1), jnp.swapaxes(coeffs, 1, 2)


def solution(mesh):
    placed = (P("row", "col"), P("col"), P(None, "col"))
    return jax.shard_map(
        shards, mesh=mesh, in_specs=placed, out_specs=(P(None, None, "col"), P()), check_vma=False
    )
```
